32 devices in a mesh: dp: 2 (over x), ep: 4 (over z), tp: 4 (over y, core).
Axes of the slice: x: 2, y: 2, z: 4, core: 2. Of those that a mesh axis runs over, the one named last changes fastest.
Arguments:
- x: bfloat16 [2048, 2048], P(('dp', 'ep')), parts along dimension 0
- idx: int32 [2048, 6], P(('dp', 'ep')), parts along dimension 0
- g: float32 [2048, 6], P(('dp', 'ep')), parts along dimension 0
- w1: bfloat16 [64, 2048, 1408], P('ep', None, 'tp')
- w3: bfloat16 [64, 2048, 1408], P('ep', None, 'tp')
- w2: bfloat16 [64, 1408, 2048], P('ep', 'tp')
Outputs:
- output: bfloat16 [2048, 2048], P(('dp', 'ep')), parts along dimension 0
There are 2 independent parts. The reference program is written for one: setup_inputs(seed, part) draws one part's arguments, and reference() takes and returns one part's arrays. A program takes and returns all parts, laid end to end along the dimension named above; an argument that names none is the same for every part.
All inputs are finite; a program needn't handle non-finite values.
Results may differ from the reference program's by a relative error of at most 0.0100673.
Values are sent between devices in bfloat16 or wider.
A program may use at most 1 GiB of HBM per device.

```python
import jax
import jax.numpy as jnp
from jax import lax

D = 2048
F = 1408
E = 64
K = 6
TL = 256
EP = 4
CF = 2
C = CF * K * TL // E
T = EP * TL


def _weights(key, shape, fan_in):
    keys = jax.random.split(key, E)
    return lax.map(lambda k: (jax.random.normal(k, shape, jnp.float32) * fan_in ** -0.5).astype(jnp.bfloat16), keys)


def _draw_route(key, part):
    src_rank = jnp.arange(T, dtype=jnp.int32) // TL
    expert_ids = jnp.arange(E, dtype=jnp.int32)
    offset = (expert_ids[None, :] + 5 * src_rank[:, None] + 3 * part) % E
    rev_rank = (E - 1) - offset
    shift_q = rev_rank // 30
    remain = rev_rank % 30
    inv_weight = ((256 << shift_q) + ((256 << shift_q) * remain) // 30).astype(jnp.uint32)
    noise_bits = jax.random.bits(key, (T, E), jnp.uint32)
    lead_zero = jnp.zeros((T, E), jnp.uint32)
    for shift_n in range(32):
        lead_zero = lead_zero + (noise_bits < jnp.uint32(1 << (31 - shift_n))).astype(jnp.uint32)
    expo_int = lead_zero * 256 + (noise_bits & 255)
    wait_score = (expo_int * inv_weight) * E + expert_ids.astype(jnp.uint32)[None, :]
    return jnp.argsort(wait_score, axis=1)[:, :K].astype(jnp.int32)


def setup_inputs(seed: int = 0, part: int = 0) -> dict:
    kshared, kparts = jax.random.split(jax.random.key(seed))
    kx, ki, kg = jax.random.split(jax.random.fold_in(kparts, part), 3)
    k1, k3, k2 = jax.random.split(kshared, 3)
    x = jax.random.normal(kx, (T, D), jnp.float32).astype(jnp.bfloat16)
    idx = _draw_route(jax.random.fold_in(ki, 7), part)
    g = jax.nn.softmax(jax.random.normal(kg, (T, K), jnp.float32), axis=-1)
    w1 = _weights(k1, (D, F), D)
    w3 = _weights(k3, (D, F), D)
    w2 = _weights(k2, (F, D), F)
    return {"x": x, "idx": idx, "g": g, "w1": w1, "w3": w3, "w2": w2}


def _dest(idx_s):
    e = idx_s.reshape(-1)
    oh = jax.nn.one_hot(e, E, dtype=jnp.int32)
    slot = jnp.sum((jnp.cumsum(oh, axis=0) - oh) * oh, axis=1)
    return jnp.where(slot < C, e * C + slot, E * C)


def _expert(args):
    xe, a, b, c = args
    h1 = jnp.dot(xe, a, preferred_element_type=jnp.float32)
    h3 = jnp.dot(xe, b, preferred_element_type=jnp.float32)
    h = (jax.nn.silu(h1) * h3).astype(jnp.bfloat16)
    return jnp.dot(h, c, preferred_element_type=jnp.float32).astype(jnp.bfloat16)


def reference(x, idx, g, w1, w3, w2):
    dest = jax.vmap(_dest)(idx.reshape(EP, TL, K))
    xr = jnp.repeat(x.reshape(EP, TL, D), K, axis=1)
    buf = jax.vmap(lambda a, d: jnp.zeros((E * C, D), a.dtype).at[d].set(a, mode="drop"))(xr, dest)
    xe = buf.reshape(EP, E, C, D).transpose(1, 0, 2, 3).reshape(E, EP * C, D)
    ye = lax.map(_expert, (xe, w1, w3, w2))
    yb = ye.reshape(E, EP, C, D).transpose(1, 0, 2, 3).reshape(EP, E * C, D)
    yc = jax.vmap(lambda a, d: jnp.take(a, d, axis=0, mode="fill", fill_value=0))(yb, dest)
    out = jnp.sum(yc.reshape(EP, TL, K, D).astype(jnp.float32) * g.reshape(EP, TL, K, 1), axis=2)
    return out.reshape(T, D).astype(jnp.bfloat16)
```

```python
import functools

import jax
import jax.numpy as jnp
from jax import lax
from jax.experimental import pallas as pl
from jax.experimental.pallas import tpu as pltpu
from jax.sharding import PartitionSpec as P

MESH = pl.DeviceIdType.MESH
CF = 2
BF = jnp.bfloat16
F32 = jnp.float32
VMEM_LIMIT = 64 * 1000 * 1000


def _peers():
    z, t = lax.axis_index("ep"), lax.axis_index("tp")
    zs = (3 - z, lax.rem(z + 2, 4), z + 1 - 2 * lax.rem(z, 2))
    yq = lax.rem(t + 2, 4)
    cq = t + 1 - 2 * lax.rem(t, 2)
    return z, t, zs, yq, cq


def _entry_barrier(zs, yq, cq):
    bar = pltpu.get_barrier_semaphore()
    for p in zs:
        pl.semaphore_signal(bar, inc=1, device_id={"ep": p}, device_id_type=MESH)
    for p in (yq, cq):
        pl.semaphore_signal(bar, inc=1, device_id={"tp": p}, device_id_type=MESH)
    pl.semaphore_wait(bar, 5)


def _rcopy(src, dst, ss, rs, dev):
    return pltpu.make_async_remote_copy(
        src_ref=src, dst_ref=dst, send_sem=ss, recv_sem=rs, device_id=dev, device_id_type=MESH
    )


def _gather_kernel(x_ref, rt_ref, xall_ref, rtall_ref, xb, rb, sem, lsem, rsem):
    z, t, zs, yq, cq = _peers()
    nr = x_ref.shape[0] // 4
    own = pltpu.make_async_copy(x_ref, xb.at[z], lsem.at[0])
    own.start()
    ownr = pltpu.make_async_copy(rt_ref, rb.at[z], lsem.at[1])
    ownr.start()
    _entry_barrier(zs, yq, cq)
    own.wait()
    ownr.wait()

    def rows(s, q):
        return xb.at[s, pl.ds(pl.multiple_of(q * nr, nr), nr)]

    zc, rc = [], []
    for i, p in enumerate(zs):
        c = _rcopy(rows(z, t), rows(z, t), sem.at[0, i], sem.at[1, i], {"ep": p})
        c.start()
        zc.append(c)
        r = _rcopy(rb.at[z], rb.at[z], rsem.at[0, i], rsem.at[1, i], {"ep": p})
        r.start()
        rc.append(r)
    yc, dc, ec = [], [], []
    for i, p in enumerate(zs):
        zc[i].wait_recv()
        c = _rcopy(rows(p, t), rows(p, t), sem.at[2, i], sem.at[3, i], {"tp": yq})
        c.start()
        yc.append(c)
        c = _rcopy(rows(p, t), rows(p, t), sem.at[4, i], sem.at[5, i], {"tp": cq})
        c.start()
        dc.append(c)
    for i, p in enumerate(zs):
        yc[i].wait_recv()
        c = _rcopy(rows(p, yq), rows(p, yq), sem.at[6, i], sem.at[7, i], {"tp": cq})
        c.start()
        ec.append(c)
    for c in rc:
        c.wait()
    for i in range(3):
        dc[i].wait_recv()
        ec[i].wait_recv()
    o = pltpu.make_async_copy(xb, xall_ref, lsem.at[0])
    o.start()
    rtall_ref[...] = rb[...]
    for c in zc + yc + dc + ec:
        c.wait_send()
    o.wait()


def _members(rt, el, ebase, k):
    tl = rt.shape[1]
    eid = lax.broadcasted_iota(jnp.int32, (el, tl), 0) + ebase
    m = jnp.zeros((el, tl), F32)
    gm = jnp.zeros((el, tl), F32)
    for j in range(k):
        hit = rt[j : j + 1, :].astype(jnp.int32) == eid
        m = jnp.where(hit, 1.0, m)
        gm = jnp.where(hit, rt[8 + j : 9 + j, :], gm)
    a = lax.broadcasted_iota(jnp.int32, (tl, tl), 0)
    b = lax.broadcasted_iota(jnp.int32, (tl, tl), 1)
    u = jnp.where(a < b, 1.0, 0.0).astype(BF)
    slot = jnp.dot(m.astype(BF), u, preferred_element_type=F32)
    return jnp.where(m > 0, slot, -1.0), gm


def _expert_kernel(k, cap, rt_ref, x_ref, w1_ref, w3_ref, h_ref, xe, pm):
    e = pl.program_id(0)
    el = xe.shape[0]
    ns, tl, d = x_ref.shape
    ebase = lax.axis_index("ep") * el

    @pl.when(e == 0)
    def _():
        ci = lax.broadcasted_iota(jnp.int32, (cap, tl), 0).astype(F32)

        @pl.loop(0, ns)
        def _(s):
            slot, _g = _members(rt_ref[s], el, ebase, k)
            for i in range(el):
                pm[i * cap : (i + 1) * cap, :] = jnp.where(slot[i : i + 1, :] == ci, 1.0, 0.0).astype(BF)

            @pl.loop(0, d // 256)
            def _(n):
                cs = pl.ds(pl.multiple_of(n * 256, 256), 256)
                v = jnp.dot(pm[...], x_ref[s, :, cs], preferred_element_type=F32).astype(BF)
                xe[:, pl.ds(pl.multiple_of(s * cap, cap), cap), cs] = v.reshape(el, cap, 256)

    xv = xe[e]
    a = jnp.dot(xv, w1_ref[0], preferred_element_type=F32)
    b = jnp.dot(xv, w3_ref[0], preferred_element_type=F32)
    h_ref[0] = (jax.nn.silu(a) * b).astype(BF)


NB = 256


def _combine_kernel(k, cap, rt_ref, h_ref, w2_ref, y_ref, gt, w2b, ypb, part, drecv, ysend, yrecv, zrecv, yb, wsem, dsem, ysem, zsem, fsem):
    z, t, zs, yq, cq = _peers()
    el, ns = h_ref.shape[0], rt_ref.shape[0]
    tl = rt_ref.shape[2]
    ebase = z * el
    sord = zs + (z,)
    own4 = (lax.rem(cq + 2, 4), yq, cq, t)
    cols = [own4[kd] * 512 + n * NB for n in range(2) for kd in range(4)]

    def wcopy(b):
        return pltpu.make_async_copy(
            w2_ref.at[:, :, pl.ds(pl.multiple_of(cols[b], NB), NB)], w2b.at[b % 2], wsem.at[b % 2]
        )

    wcopy(0).start()
    _entry_barrier(zs, yq, cq)

    ci = lax.broadcasted_iota(jnp.int32, (cap, tl), 0).astype(F32)

    @pl.loop(0, ns)
    def _(s):
        slot, gm = _members(rt_ref[s], el, ebase, k)
        gf = jnp.concatenate(
            [jnp.where(slot[i : i + 1, :] == ci, gm[i : i + 1, :], 0.0) for i in range(el)], axis=0
        )
        g = gf.T
        hi = g.astype(BF)
        r = g - hi.astype(F32)
        mid = r.astype(BF)
        gt[s, 0] = hi
        gt[s, 1] = mid
        gt[s, 2] = (r - mid.astype(F32)).astype(BF)

    def compute(b):
        wcopy(b).wait()
        if b + 1 < 8:
            wcopy(b + 1).start()
        sl = b % 2

        @pl.loop(0, el, step=4)
        def _(e0):
            for i in range(4):
                e = e0 + i
                v = jnp.dot(h_ref[e], w2b[sl, e], preferred_element_type=F32).astype(BF)
                ypb[:, pl.ds(pl.multiple_of(e * cap, cap), cap), :] = v.reshape(ns, cap, NB)

        @pl.loop(0, ns)
        def _(s):
            yp = ypb[s]
            acc = jnp.dot(gt[s, 0], yp, preferred_element_type=F32)
            acc += jnp.dot(gt[s, 1], yp, preferred_element_type=F32)
            acc += jnp.dot(gt[s, 2], yp, preferred_element_type=F32)
            part[b, s] = acc

    def dcopy(n, j):
        return _rcopy(part.at[n * 4 + 2 * j], drecv.at[n, j], dsem.at[0, n, j], dsem.at[1, n, j], {"tp": cq})

    def ycopy(n, i):
        return _rcopy(ysend.at[n, sord[i]], yrecv.at[n, sord[i]], ysem.at[0, n, i], ysem.at[1, n, i], {"tp": yq})

    def zcopy(n, i):
        return _rcopy(ysend.at[n, 4 + i], zrecv.at[n, i], zsem.at[0, n, i], zsem.at[1, n, i], {"ep": zs[i]})

    def ystep(n):
        dcopy(n, 0).wait_recv()
        for i in range(4):
            s = sord[i]
            ysend[n, s] = part[n * 4 + 1, s] + drecv[n, 0, s]
        for i in range(4):
            ycopy(n, i).start()

    def zstep(n, i):
        s = sord[i]
        ycopy(n, i).wait_recv()
        ysend[n, 4 + i] = part[n * 4 + 3, s] + drecv[n, 1, s] + yrecv[n, s]
        if i < 3:
            zcopy(n, i).start()

    def fcopy(j, n, q, dev):
        sl = pl.ds(pl.multiple_of(q * 512 + n * NB, NB), NB)
        return _rcopy(yb.at[:, sl], yb.at[:, sl], fsem.at[0, n, j], fsem.at[1, n, j], {"tp": dev})

    def finish(n):
        acc = ysend[n, 7]
        for i in range(3):
            zcopy(n, i).wait_recv()
            acc += zrecv[n, i]
        yb[:, pl.ds(pl.multiple_of(t * 512 + n * NB, NB), NB)] = acc.astype(BF)

    def spread(n):
        fcopy(0, n, t, yq).start()
        fcopy(1, n, t, cq).start()

    compute(0)
    dcopy(0, 0).start()
    compute(1)
    ystep(0)
    compute(2)
    dcopy(0, 1).start()
    compute(3)
    dcopy(0, 1).wait_recv()
    zstep(0, 0)
    compute(4)
    dcopy(1, 0).start()
    compute(5)
    ystep(1)
    zstep(0, 1)
    compute(6)
    dcopy(1, 1).start()
    zstep(0, 2)
    compute(7)
    dcopy(1, 1).wait_recv()
    zstep(0, 3)
    zstep(1, 0)
    zstep(1, 1)
    finish(0)
    zstep(1, 2)
    spread(0)
    zstep(1, 3)
    finish(1)
    spread(1)
    for n in range(2):
        fcopy(0, n, t, yq).wait_recv()
        fcopy(2, n, yq, cq).start()
    for n in range(2):
        for j in range(2):
            dcopy(n, j).wait_send()
        for i in range(4):
            ycopy(n, i).wait_send()
        for i in range(3):
            zcopy(n, i).wait_send()
    for n in range(2):
        fcopy(1, n, t, cq).wait_recv()
        fcopy(2, n, yq, cq).wait_recv()
        for j in range(3):
            fcopy(j, n, t, cq).wait_send()
    y_ref[...] = yb[...]


def solution(mesh):
    tok = P(("dp", "ep"), None)
    nep = mesh.shape["ep"]

    def body(x, idx, g, w1, w3, w2):
        tl, d = x.shape
        k = idx.shape[1]
        el, _, fl = w1.shape
        cap = CF * k * tl // (el * nep)
        pad = jnp.zeros((8 - k, tl), F32)
        rt = jnp.concatenate([idx.T.astype(F32), pad, g.T, pad], axis=0)
        vm = pl.BlockSpec(memory_space=pltpu.VMEM)
        hbm = pl.BlockSpec(memory_space=pl.ANY)
        dma = pltpu.SemaphoreType.DMA
        xall, rtall = pl.pallas_call(
            _gather_kernel,
            out_shape=(jax.ShapeDtypeStruct((nep, tl, d), BF), jax.ShapeDtypeStruct((nep, 16, tl), F32)),
            in_specs=[hbm, hbm],
            out_specs=(hbm, vm),
            scratch_shapes=[
                pltpu.VMEM((nep, tl, d), BF),
                pltpu.VMEM((nep, 16, tl), F32),
                dma((8, 3)),
                dma((2,)),
                dma((2, 3)),
            ],
            compiler_params=pltpu.CompilerParams(collective_id=0, has_side_effects=True),
        )(x, rt)
        h = pl.pallas_call(
            functools.partial(_expert_kernel, k, cap),
            grid=(el,),
            out_shape=jax.ShapeDtypeStruct((el, nep * cap, fl), BF),
            in_specs=[
                pl.BlockSpec((nep, 16, tl), lambda e: (0, 0, 0)),
                pl.BlockSpec((nep, tl, d), lambda e: (0, 0, 0)),
                pl.BlockSpec((1, d, fl), lambda e: (e, 0, 0)),
                pl.BlockSpec((1, d, fl), lambda e: (e, 0, 0)),
            ],
            out_specs=pl.BlockSpec((1, nep * cap, fl), lambda e: (e, 0, 0)),
            scratch_shapes=[pltpu.VMEM((el, nep * cap, d), BF), pltpu.VMEM((el * cap, tl), BF)],
            compiler_params=pltpu.CompilerParams(vmem_limit_bytes=VMEM_LIMIT),
        )(rtall, xall, w1, w3)
        y = pl.pallas_call(
            functools.partial(_combine_kernel, k, cap),
            out_shape=jax.ShapeDtypeStruct((tl, d), BF),
            in_specs=[vm, vm, hbm],
            out_specs=vm,
            scratch_shapes=[
                pltpu.VMEM((nep, 3, tl, el * cap), BF),
                pltpu.VMEM((2, el, fl, NB), BF),
                pltpu.VMEM((nep, el * cap, NB), BF),
                pltpu.VMEM((8, nep, tl, NB), F32),
                pltpu.VMEM((2, 2, nep, tl, NB), F32),
                pltpu.VMEM((2, 8, tl, NB), F32),
                pltpu.VMEM((2, nep, tl, NB), F32),
                pltpu.VMEM((2, 3, tl, NB), F32),
                pltpu.VMEM((tl, d), BF),
                dma((2,)),
                dma((2, 2, 2)),
                dma((2, 2, 4)),
                dma((2, 2, 3)),
                dma((2, 2, 3)),
            ],
            compiler_params=pltpu.CompilerParams(
                collective_id=1, has_side_effects=True, vmem_limit_bytes=VMEM_LIMIT
            ),
        )(rtall, h, w2)
        return y

    return jax.shard_map(
        body,
        mesh=mesh,
        in_specs=(tok, tok, tok, P("ep", None, "tp"), P("ep", None, "tp"), P("ep", "tp", None)),
        out_specs=tok,
        check_vma=False,
    )
```

```python
import functools

import jax
import jax.numpy as jnp
from jax import lax
from jax.experimental import pallas as pl
from jax.experimental.pallas import tpu as pltpu
from jax.sharding import PartitionSpec as P

MESH = pl.DeviceIdType.MESH
CF = 2
BF = jnp.bfloat16
F32 = jnp.float32
VMEM_LIMIT = 64 * 1000 * 1000


def _peers():
    z, t = lax.axis_index("ep"), lax.axis_index("tp")
    zs = (3 - z, lax.rem(z + 2, 4), z + 1 - 2 * lax.rem(z, 2))
    yq = lax.rem(t + 2, 4)
    cq = t + 1 - 2 * lax.rem(t, 2)
    return z, t, zs, yq, cq


def _entry_barrier(zs, yq, cq):
    bar = pltpu.get_barrier_semaphore()
    for p in zs:
        pl.semaphore_signal(bar, inc=1, device_id={"ep": p}, device_id_type=MESH)
    for p in (yq, cq):
        pl.semaphore_signal(bar, inc=1, device_id={"tp": p}, device_id_type=MESH)
    pl.semaphore_wait(bar, 5)


def _rcopy(src, dst, ss, rs, dev):
    return pltpu.make_async_remote_copy(
        src_ref=src, dst_ref=dst, send_sem=ss, recv_sem=rs, device_id=dev, device_id_type=MESH
    )


def _members(rt, el, ebase, k):
    tl = rt.shape[1]
    eid = lax.broadcasted_iota(jnp.int32, (el, tl), 0) + ebase
    m = jnp.zeros((el, tl), F32)
    gm = jnp.zeros((el, tl), F32)
    for j in range(k):
        hit = rt[j : j + 1, :].astype(jnp.int32) == eid
        m = jnp.where(hit, 1.0, m)
        gm = jnp.where(hit, rt[8 + j : 9 + j, :], gm)
    a = lax.broadcasted_iota(jnp.int32, (tl, tl), 0)
    b = lax.broadcasted_iota(jnp.int32, (tl, tl), 1)
    u = jnp.where(a < b, 1.0, 0.0).astype(BF)
    slot = jnp.dot(m.astype(BF), u, preferred_element_type=F32)
    return jnp.where(m > 0, slot, -1.0), gm


NB = 256
UN = 256
EB = 4
SL = 4
NT = (((1,), (1,)), ((), ()))


def _moe_kernel(
    k, cap, x_ref, id_ref, g_ref, w1_ref, w3_ref, w2_ref, y_ref,
    xb, rb, pm, gt, xe, hacc, hb, wb, w2b, ypb, part, drecv, yrecv, zrecv, yb,
    lsem, rsem, xsem, wsem, w2sem, dsem, ysem, zsem, zrsem, fsem,
):
    z, t, zs, yq, cq = _peers()
    ns, tl, d = xb.shape
    el, fl = hb.shape[0], hb.shape[2]
    ebase = z * el
    nr = tl // 4
    nu = d // UN
    ng = el // EB
    side = z // 2
    inner = (z == 1) | (z == 2)

    def wcopies(step):
        c, g = step // ng, lax.rem(step, ng)
        sl = lax.rem(step, SL)
        cs = pl.ds(pl.multiple_of(c * UN, UN), UN)
        es = pl.ds(g * EB, EB)
        return (
            pltpu.make_async_copy(w1_ref.at[es, :, cs], wb.at[sl, :, pl.ds(0, fl)], wsem.at[0, sl]),
            pltpu.make_async_copy(w3_ref.at[es, :, cs], wb.at[sl, :, pl.ds(fl, fl)], wsem.at[1, sl]),
        )

    def wstart(step):
        for c in wcopies(step):
            c.start()

    own4 = (lax.rem(cq + 2, 4), yq, cq, t)
    cols = [own4[kd] * 512 + n * NB for n in range(2) for kd in range(4)]

    def w2copy(b):
        return pltpu.make_async_copy(
            w2_ref.at[:, :, pl.ds(pl.multiple_of(cols[b], NB), NB)], w2b.at[b % 2], w2sem.at[b % 2]
        )

    own = pltpu.make_async_copy(x_ref, xb.at[z], lsem.at[0])
    own.start()
    rb[z, 0:k] = id_ref[...].astype(F32)
    rb[z, 8 : 8 + k] = g_ref[...]
    for step in range(SL - 1):
        wstart(step)
    _entry_barrier(zs, yq, cq)
    own.wait()

    def piece(c, s, q):
        return xb.at[s, pl.ds(pl.multiple_of(q * nr, nr), nr), pl.ds(pl.multiple_of(c * UN, UN), UN)]

    def xcopy(kind, c, i):
        p = zs[i]
        if kind == 0:
            r, dev = piece(c, z, t), {"ep": p}
        elif kind == 1:
            r, dev = piece(c, p, t), {"tp": yq}
        elif kind == 2:
            r, dev = piece(c, p, t), {"tp": cq}
        else:
            r, dev = piece(c, p, yq), {"tp": cq}
        return _rcopy(r, r, xsem.at[2 * kind, c, i], xsem.at[2 * kind + 1, c, i], dev)

    def rcopy(i):
        return _rcopy(rb.at[z], rb.at[z], rsem.at[0, i], rsem.at[1, i], {"ep": zs[i]})

    for i in range(3):
        rcopy(i).start()

    @pl.loop(0, nu)
    def _(c):
        for i in range(3):
            xcopy(0, c, i).start()

    def zforward(c):
        for i in range(3):
            xcopy(0, c, i).wait_recv()
            xcopy(1, c, i).start()
            xcopy(2, c, i).start()

    def yforward(c):
        for i in range(3):
            xcopy(1, c, i).wait_recv()
            xcopy(3, c, i).start()

    def xarrive(c):
        for i in range(3):
            xcopy(2, c, i).wait_recv()
            xcopy(3, c, i).wait_recv()

    ci = lax.broadcasted_iota(jnp.int32, (cap, tl), 0).astype(F32)

    def tables(s):
        slot, gm = _members(rb[s], el, ebase, k)
        gs = []
        for i in range(el):
            hit = slot[i : i + 1, :] == ci
            pm[s, i * cap : (i + 1) * cap, :] = jnp.where(hit, 1.0, 0.0).astype(BF)
            gs.append(jnp.where(hit, gm[i : i + 1, :], 0.0))
        g = jnp.concatenate(gs, axis=0).T
        hi = g.astype(BF)
        r = g - hi.astype(F32)
        mid = r.astype(BF)
        gt[s, 0] = hi
        gt[s, 1] = mid
        gt[s, 2] = (r - mid.astype(F32)).astype(BF)

    @pl.loop(0, el)
    def _(e):
        hacc[e] = jnp.zeros(hacc.shape[1:], F32)

    zforward(0)
    for i in range(3):
        rcopy(i).wait_recv()

    @pl.loop(0, 2)
    def _(s):
        tables(s)

    zforward(1)

    @pl.loop(2, 4)
    def _(s):
        tables(s)

    yforward(0)

    @pl.loop(0, nu)
    def _(c):
        @pl.when(c < nu - 2)
        def _():
            zforward(c + 2)

        @pl.when(c < nu - 1)
        def _():
            yforward(c + 1)

        xarrive(c)
        cs = pl.ds(pl.multiple_of(c * UN, UN), UN)

        @pl.loop(0, ns)
        def _(s):
            v = jnp.dot(pm[s], xb[s, :, cs], preferred_element_type=F32).astype(BF)
            xe[:, pl.ds(pl.multiple_of(s * cap, cap), cap), :] = v.reshape(el, cap, UN)

        @pl.loop(0, ng)
        def _(g):
            step = c * ng + g
            for w in wcopies(step):
                w.wait()

            @pl.when(step + SL - 1 < nu * ng)
            def _():
                wstart(step + SL - 1)

            sl = lax.rem(step, SL)
            for i in range(EB):
                e = g * EB + i
                hacc[e] += lax.dot_general(xe[e], wb[sl, i], NT, preferred_element_type=F32)

    w2copy(0).start()

    @pl.loop(0, el)
    def _(e):
        ab = hacc[e]
        hb[e] = (jax.nn.silu(ab[:, :fl]) * ab[:, fl:]).astype(BF)

    def sof(i):
        far = (3 - i) * (1 - side) + i * side
        near = (i - 2) * z + (3 - i) * (1 - z + 4 * side)
        return far * (1 - i // 2) + near * (i // 2)

    def dcopy(n, j, i):
        s = sof(i)
        return _rcopy(
            part.at[n * 4 + 2 * j, s], drecv.at[n, j, s], dsem.at[0, n, j, i], dsem.at[1, n, j, i], {"tp": cq}
        )

    def ycopy(n, i):
        s = sof(i)
        return _rcopy(part.at[n * 4 + 1, s], yrecv.at[n, s], ysem.at[0, n, i], ysem.at[1, n, i], {"tp": yq})

    def compute(n, kd):
        b = n * 4 + kd
        w2copy(b).wait()
        if b + 1 < 8:
            w2copy(b + 1).start()
        sl = b % 2

        @pl.loop(0, el, step=EB)
        def _(e0):
            for i in range(EB):
                e = e0 + i
                v = jnp.dot(hb[e], w2b[sl, e], preferred_element_type=F32).astype(BF)
                ypb[:, pl.ds(pl.multiple_of(e * cap, cap), cap), :] = v.reshape(ns, cap, NB)

        @pl.loop(0, ns)
        def _(i):
            s = sof(i)
            yp = ypb[s]
            acc = jnp.dot(gt[s, 0], yp, preferred_element_type=F32)
            acc += jnp.dot(gt[s, 1], yp, preferred_element_type=F32)
            acc += jnp.dot(gt[s, 2], yp, preferred_element_type=F32)
            if kd % 2 == 0:
                part[b, s] = acc
                dcopy(n, kd // 2, i).start()
            else:
                dcopy(n, kd // 2, i).wait_recv()
                part[b, s] = acc + drecv[n, kd // 2, s]
                if kd == 1:

                    @pl.when(i < 3)
                    def _():
                        ycopy(n, i).start()

    def zcopy(n, i):
        s = sof(i)
        if i < 2:
            dr = side
        else:
            dr = lax.rem(z, 2)
        return _rcopy(
            part.at[n * 4 + 3, s], zrecv.at[n, dr * 4 + s], zsem.at[n, i], zrsem.at[n, dr * 4 + s], {"ep": z + 1 - 2 * dr}
        ), zrecv.at[n, dr * 4 + s]

    def zacc(n, i):
        s = sof(i)
        ycopy(n, i).wait_recv()
        part[n * 4 + 3, s] += yrecv[n, s]
        if i < 3:

            @pl.when(~inner)
            def _():
                zcopy(n, i)[0].start()

    def relay(n, i):
        @pl.when(inner)
        def _():
            c, buf = zcopy(n, i)
            c.wait_recv()
            part[n * 4 + 3, sof(i)] += buf[...]
            c.start()

    def zarrive(n, dr):
        _rcopy(
            part.at[n * 4 + 3, z], zrecv.at[n, dr * 4 + z], zsem.at[n, 0], zrsem.at[n, dr * 4 + z], {"ep": zs[0]}
        ).wait_recv()
        part[n * 4 + 3, z] += zrecv[n, dr * 4 + z]

    def fcopy(j, n):
        q, dev = ((t, yq), (t, cq), (yq, cq))[j]
        sl = pl.ds(pl.multiple_of(q * 512 + n * NB, NB), NB)
        return _rcopy(yb.at[:, sl], yb.at[:, sl], fsem.at[0, n, j], fsem.at[1, n, j], {"tp": dev})

    def finish(n):
        @pl.when(z > 0)
        def _():
            zarrive(n, 0)

        @pl.when(z < 3)
        def _():
            zarrive(n, 1)

        yb[:, pl.ds(pl.multiple_of(t * 512 + n * NB, NB), NB)] = part[n * 4 + 3, z].astype(BF)

    def spread(n):
        fcopy(0, n).start()
        fcopy(1, n).start()

    compute(0, 0)
    compute(0, 1)
    compute(0, 2)
    compute(0, 3)
    zacc(0, 0)
    compute(1, 0)
    zacc(0, 1)
    compute(1, 1)
    ycopy(0, 3).start()
    ycopy(1, 3).start()
    relay(0, 0)
    compute(1, 2)
    zacc(0, 2)
    compute(1, 3)
    relay(0, 1)
    zacc(1, 0)
    relay(0, 2)
    zacc(1, 1)
    relay(1, 0)
    zacc(1, 2)
    relay(1, 1)
    zacc(0, 3)
    relay(1, 2)
    finish(0)
    spread(0)
    zacc(1, 3)
    finish(1)
    spread(1)
    for n in range(2):
        fcopy(0, n).wait_recv()
        fcopy(2, n).start()

    @pl.loop(0, nu)
    def _(c):
        for kind in range(4):
            for i in range(3):
                xcopy(kind, c, i).wait_send()

    for i in range(3):
        rcopy(i).wait_send()
    for n in range(2):
        for i in range(4):
            for j in range(2):
                dcopy(n, j, i).wait_send()
            ycopy(n, i).wait_send()
            if i < 3:
                zcopy(n, i)[0].wait_send()
    for n in range(2):
        fcopy(1, n).wait_recv()
        fcopy(2, n).wait_recv()
    for n in range(2):
        for j in range(3):
            fcopy(j, n).wait_send()
    y_ref[...] = yb[...]


def solution(mesh):
    tok = P(("dp", "ep"), None)
    nep = mesh.shape["ep"]

    def body(x, idx, g, w1, w3, w2):
        tl, d = x.shape
        k = idx.shape[1]
        el, _, fl = w1.shape
        cap = CF * k * tl // (el * nep)
        vm = pl.BlockSpec(memory_space=pltpu.VMEM)
        hbm = pl.BlockSpec(memory_space=pl.ANY)
        dma = pltpu.SemaphoreType.DMA
        nu = d // UN
        return pl.pallas_call(
            functools.partial(_moe_kernel, k, cap),
            out_shape=jax.ShapeDtypeStruct((tl, d), BF),
            in_specs=[hbm, vm, vm, hbm, hbm, hbm],
            out_specs=vm,
            scratch_shapes=[
                pltpu.VMEM((nep, tl, d), BF),
                pltpu.VMEM((nep, 16, tl), F32),
                pltpu.VMEM((nep, el * cap, tl), BF),
                pltpu.VMEM((nep, 3, tl, el * cap), BF),
                pltpu.VMEM((el, nep * cap, UN), BF),
                pltpu.VMEM((el, nep * cap, 2 * fl), F32),
                pltpu.VMEM((el, nep * cap, fl), BF),
                pltpu.VMEM((SL, EB, 2 * fl, UN), BF),
                pltpu.VMEM((2, el, fl, NB), BF),
                pltpu.VMEM((nep, el * cap, NB), BF),
                pltpu.VMEM((8, nep, tl, NB), F32),
                pltpu.VMEM((2, 2, nep, tl, NB), F32),
                pltpu.VMEM((2, nep, tl, NB), F32),
                pltpu.VMEM((2, 8, tl, NB), F32),
                pltpu.VMEM((tl, d), BF),
                dma((1,)),
                dma((2, 3)),
                dma((8, nu, 3)),
                dma((2, SL)),
                dma((2,)),
                dma((2, 2, 2, 4)),
                dma((2, 2, 4)),
                dma((2, 3)),
                dma((2, 8)),
                dma((2, 2, 3)),
            ],
            compiler_params=pltpu.CompilerParams(
                collective_id=0, has_side_effects=True, vmem_limit_bytes=VMEM_LIMIT
            ),
        )(x, idx.T, g.T, w1.swapaxes(1, 2), w3.swapaxes(1, 2), w2)

    return jax.shard_map(
        body,
        mesh=mesh,
        in_specs=(tok, tok, tok, P("ep", None, "tp"), P("ep", None, "tp"), P("ep", "tp", None)),
        out_specs=tok,
        check_vma=False,
    )
```

```python
import functools

import jax
import jax.numpy as jnp
from jax import lax
from jax.experimental import pallas as pl
from jax.experimental.pallas import tpu as pltpu
from jax.sharding import PartitionSpec as P

MESH = pl.DeviceIdType.MESH
CF = 2
BF = jnp.bfloat16
F32 = jnp.float32
VMEM_LIMIT = 64 * 1000 * 1000


def _peers():
    z, t = lax.axis_index("ep"), lax.axis_index("tp")
    zs = (3 - z, lax.rem(z + 2, 4), z + 1 - 2 * lax.rem(z, 2))
    yq = lax.rem(t + 2, 4)
    cq = t + 1 - 2 * lax.rem(t, 2)
    return z, t, zs, yq, cq


def _entry_barrier(zs, yq, cq):
    bar = pltpu.get_barrier_semaphore()
    for p in zs:
        pl.semaphore_signal(bar, inc=1, device_id={"ep": p}, device_id_type=MESH)
    for p in (yq, cq):
        pl.semaphore_signal(bar, inc=1, device_id={"tp": p}, device_id_type=MESH)
    pl.semaphore_wait(bar, 5)


def _rcopy(src, dst, ss, rs, dev):
    return pltpu.make_async_remote_copy(
        src_ref=src, dst_ref=dst, send_sem=ss, recv_sem=rs, device_id=dev, device_id_type=MESH
    )


def _members(rt, el, ebase, k):
    tl = rt.shape[1]
    eid = lax.broadcasted_iota(jnp.int32, (el, tl), 0) + ebase
    m = jnp.zeros((el, tl), F32)
    gm = jnp.zeros((el, tl), F32)
    for j in range(k):
        hit = rt[j : j + 1, :].astype(jnp.int32) == eid
        m = jnp.where(hit, 1.0, m)
        gm = jnp.where(hit, rt[8 + j : 9 + j, :], gm)
    a = lax.broadcasted_iota(jnp.int32, (tl, tl), 0)
    b = lax.broadcasted_iota(jnp.int32, (tl, tl), 1)
    u = jnp.where(a < b, 1.0, 0.0).astype(BF)
    slot = jnp.dot(m.astype(BF), u, preferred_element_type=F32)
    return jnp.where(m > 0, slot, -1.0), gm


NB = 256
UN = 256
CU = 512
EB = 4
SL = 3
NT = (((1,), (1,)), ((), ()))


def _moe_kernel(
    k, cap, x_ref, id_ref, g_ref, w1_ref, w3_ref, w2_ref, y_ref,
    xb, rb, pm, gt, xe, hacc, hb, wb, w2b, part, drecv, yrecv, zrecv, zfrecv, yb,
    lsem, rsem, xsem, wsem, w2sem, dsem, ysem, zsem, zrsem, zfsem, fsem,
):
    z, t, zs, yq, cq = _peers()
    ns, tl, d = xb.shape
    el, fl = hb.shape[0], hb.shape[2]
    ebase = z * el
    nr = tl // 4
    nu = d // UN
    nc = d // CU
    ng = el // EB
    side = z // 2
    inner = (z == 1) | (z == 2)

    def wcopies(step):
        c, g = step // ng, lax.rem(step, ng)
        sl = lax.rem(step, SL)
        cs = pl.ds(pl.multiple_of(c * CU, CU), CU)
        es = pl.ds(g * EB, EB)
        return (
            pltpu.make_async_copy(w1_ref.at[es, :, cs], wb.at[sl, :, pl.ds(0, fl)], wsem.at[0, sl]),
            pltpu.make_async_copy(w3_ref.at[es, :, cs], wb.at[sl, :, pl.ds(fl, fl)], wsem.at[1, sl]),
        )

    def wstart(step):
        for c in wcopies(step):
            c.start()

    own4 = (lax.rem(cq + 2, 4), yq, cq, t)
    cols = [own4[kd] * 512 + n * NB for n in range(2) for kd in range(4)]

    def w2copy(b):
        return pltpu.make_async_copy(
            w2_ref.at[:, :, pl.ds(pl.multiple_of(cols[b], NB), NB)], w2b.at[b % 2], w2sem.at[b % 2]
        )

    own = pltpu.make_async_copy(x_ref, xb.at[z], lsem.at[0])
    own.start()
    rb[z, 0:k] = id_ref[...].astype(F32)
    rb[z, 8 : 8 + k] = g_ref[...]
    for step in range(SL - 1):
        wstart(step)
    w2copy(0).start()
    w2copy(1).start()
    _entry_barrier(zs, yq, cq)
    own.wait()

    def piece(c, s, q):
        return xb.at[s, pl.ds(pl.multiple_of(q * nr, nr), nr), pl.ds(pl.multiple_of(c * UN, UN), UN)]

    def xcopy(kind, c, i):
        p = zs[i]
        if kind == 0:
            r, dev = piece(c, z, t), {"ep": p}
        elif kind == 1:
            r, dev = piece(c, p, t), {"tp": yq}
        elif kind == 2:
            r, dev = piece(c, p, t), {"tp": cq}
        else:
            r, dev = piece(c, p, yq), {"tp": cq}
        return _rcopy(r, r, xsem.at[2 * kind, c, i], xsem.at[2 * kind + 1, c, i], dev)

    def rcopy(i):
        return _rcopy(rb.at[z], rb.at[z], rsem.at[0, i], rsem.at[1, i], {"ep": zs[i]})

    for i in range(3):
        rcopy(i).start()

    @pl.loop(0, nu)
    def _(c):
        for i in range(3):
            xcopy(0, c, i).start()

    def zforward(c):
        for i in range(3):
            xcopy(0, c, i).wait_recv()
            xcopy(1, c, i).start()
            xcopy(2, c, i).start()

    def yforward(c):
        for i in range(3):
            xcopy(1, c, i).wait_recv()
            xcopy(3, c, i).start()

    def xarrive(c):
        for i in range(3):
            xcopy(2, c, i).wait_recv()
            xcopy(3, c, i).wait_recv()

    ci = lax.broadcasted_iota(jnp.int32, (cap, tl), 0).astype(F32)

    def tables(s):
        slot, gm = _members(rb[s], el, ebase, k)
        gs = []
        for i in range(el):
            hit = slot[i : i + 1, :] == ci
            pm[s, i * cap : (i + 1) * cap, :] = jnp.where(hit, 1.0, 0.0).astype(BF)
            gs.append(jnp.where(hit, gm[i : i + 1, :], 0.0))
        g = jnp.concatenate(gs, axis=0).T
        hi = g.astype(BF)
        r = g - hi.astype(F32)
        mid = r.astype(BF)
        gt[s, 0] = hi
        gt[s, 1] = mid
        gt[s, 2] = (r - mid.astype(F32)).astype(BF)

    @pl.loop(0, el)
    def _(e):
        hacc[e] = jnp.zeros(hacc.shape[1:], F32)

    zforward(0)
    for i in range(3):
        rcopy(i).wait_recv()

    @pl.loop(0, 2)
    def _(s):
        tables(s)

    zforward(1)

    @pl.loop(2, 4)
    def _(s):
        tables(s)

    zforward(2)
    yforward(0)
    yforward(1)
    zforward(3)

    @pl.loop(0, nc)
    def _(c):
        u = c * (CU // UN)
        xarrive(u)
        xarrive(u + 1)
        cs = pl.ds(pl.multiple_of(c * CU, CU), CU)
        for s in range(ns):
            v = jnp.dot(pm[s], xb[s, :, cs], preferred_element_type=F32).astype(BF)
            xe[:, s * cap : (s + 1) * cap, :] = v.reshape(el, cap, CU)
        for g in range(ng):
            step = c * ng + g
            if g == 1:

                @pl.when(c < nc - 1)
                def _():
                    yforward(u + 2)

            if g == 2:

                @pl.when(c < nc - 2)
                def _():
                    zforward(u + 4)

            if g == 3:

                @pl.when(c < nc - 1)
                def _():
                    yforward(u + 3)

            for w in wcopies(step):
                w.wait()

            @pl.when(step + SL - 1 < nc * ng)
            def _():
                wstart(step + SL - 1)

            sl = lax.rem(step, SL)
            for i in range(EB):
                e = g * EB + i
                hacc[e] += lax.dot_general(wb[sl, i], xe[e], NT, preferred_element_type=F32)

        @pl.when(c < nc - 2)
        def _():
            zforward(u + 5)

    @pl.loop(0, el, step=2)
    def _(e0):
        for i in range(2):
            ab = hacc[e0 + i]
            hb[e0 + i] = (jax.nn.silu(ab[:fl]) * ab[fl:]).T.astype(BF)

    def sof(i):
        far = (3 - i) * (1 - side) + i * side
        near = (i - 2) * z + (3 - i) * (1 - z + 4 * side)
        return far * (1 - i // 2) + near * (i // 2)

    def dcopy(n, j, i):
        s = sof(i)
        return _rcopy(
            part.at[n * 4 + 2 * j, s], drecv.at[n, j, s], dsem.at[0, n, j, i], dsem.at[1, n, j, i], {"tp": cq}
        )

    def ycopy(n, i):
        s = sof(i)
        return _rcopy(part.at[n * 4 + 1, s], yrecv.at[n, s], ysem.at[0, n, i], ysem.at[1, n, i], {"tp": yq})

    def zfirst():
        return _rcopy(part.at[1, sof(2)], zfrecv, zfsem.at[0], zfsem.at[1], {"ep": zs[2]})

    def compute(n, kd):
        b = n * 4 + kd
        w2copy(b).wait()
        sl = b % 2

        @pl.loop(0, el, step=8)
        def _(e0):
            for i in range(8):
                e = e0 + i
                v = jnp.dot(hb[e], w2b[sl, e], preferred_element_type=F32).astype(BF)
                pm[:, pl.ds(pl.multiple_of(e * cap, cap), cap), :] = v.reshape(ns, cap, NB)

        if b + 2 < 8:
            w2copy(b + 2).start()

        @pl.loop(0, ns)
        def _(i):
            s = sof(i)
            yp = pm[s]
            acc = jnp.dot(gt[s, 0], yp, preferred_element_type=F32)
            acc += jnp.dot(gt[s, 1], yp, preferred_element_type=F32)
            acc += jnp.dot(gt[s, 2], yp, preferred_element_type=F32)
            if kd % 2 == 0:
                part[b, s] = acc
                dcopy(n, kd // 2, i).start()
            else:
                dcopy(n, kd // 2, i).wait_recv()
                part[b, s] = acc + drecv[n, kd // 2, s]
                if kd == 1:

                    @pl.when(i < 2 + n)
                    def _():
                        ycopy(n, i).start()

                    if n == 0:

                        @pl.when(i == 2)
                        def _():
                            zfirst().start()

    def zdir(i):
        return side if i < 2 else lax.rem(z, 2)

    def zcopy(n, i):
        s, dr = sof(i), zdir(i)
        dn = z + 1 - 2 * dr
        slot = s - dn + 4 * dr
        return _rcopy(part.at[n * 4 + 3, s], zrecv.at[n, slot], zsem.at[n, i], zrsem.at[n, slot], {"ep": dn})

    def zarrive(n, s, slot):
        _rcopy(
            part.at[n * 4 + 3, s], zrecv.at[n, slot], zsem.at[n, 0], zrsem.at[n, slot], {"ep": zs[0]}
        ).wait_recv()
        part[n * 4 + 3, s] += zrecv[n, slot]

    def zacc(n, i):
        s = sof(i)
        if (n, i) != (0, 2):
            ycopy(n, i).wait_recv()
            part[n * 4 + 3, s] += yrecv[n, s]
        if i < 3:

            @pl.when(~inner)
            def _():
                zcopy(n, i).start()

    def relay(n, i):
        @pl.when(inner)
        def _():
            s = sof(i)
            zarrive(n, s, s - z + 4 * zdir(i))
            zcopy(n, i).start()

    def fcopy(j, n):
        q, dev = ((t, yq), (t, cq), (yq, cq))[j]
        sl = pl.ds(pl.multiple_of(q * 512 + n * NB, NB), NB)
        return _rcopy(yb.at[:, sl], yb.at[:, sl], fsem.at[0, n, j], fsem.at[1, n, j], {"tp": dev})

    def finish(n):
        @pl.when(z > 0)
        def _():
            zarrive(n, z, 0)

        @pl.when(z < 3)
        def _():
            zarrive(n, z, 4)

        yb[:, pl.ds(pl.multiple_of(t * 512 + n * NB, NB), NB)] = part[n * 4 + 3, z].astype(BF)

    def spread(n):
        fcopy(0, n).start()
        fcopy(1, n).start()

    compute(0, 0)
    compute(0, 1)
    compute(0, 2)
    compute(0, 3)
    zacc(0, 2)
    zacc(0, 0)
    compute(1, 0)
    zacc(0, 1)
    compute(1, 1)
    zfirst().wait_recv()
    part[1, z] += zfrecv[...]
    ycopy(0, 3).start()
    ycopy(1, 3).start()
    relay(0, 0)
    compute(1, 2)
    compute(1, 3)
    relay(0, 1)
    zacc(1, 0)
    zacc(1, 1)
    relay(0, 2)
    relay(1, 0)
    zacc(1, 2)
    relay(1, 1)
    zacc(0, 3)
    relay(1, 2)
    finish(0)
    spread(0)
    zacc(1, 3)
    finish(1)
    spread(1)
    for n in range(2):
        fcopy(0, n).wait_recv()
        fcopy(2, n).start()

    @pl.loop(0, nu)
    def _(c):
        for kind in range(4):
            for i in range(3):
                xcopy(kind, c, i).wait_send()

    for i in range(3):
        rcopy(i).wait_send()
    for n in range(2):
        for i in range(4):
            for j in range(2):
                dcopy(n, j, i).wait_send()
            if (n, i) != (0, 2):
                ycopy(n, i).wait_send()
            if i < 3:
                zcopy(n, i).wait_send()
    zfirst().wait_send()
    for n in range(2):
        fcopy(1, n).wait_recv()
        fcopy(2, n).wait_recv()
    for n in range(2):
        for j in range(3):
            fcopy(j, n).wait_send()
    out = pltpu.make_async_copy(yb, y_ref, lsem.at[0])
    out.start()
    out.wait()


def solution(mesh):
    tok = P(("dp", "ep"), None)
    nep = mesh.shape["ep"]

    def body(x, idx, g, w1, w3, w2):
        tl, d = x.shape
        k = idx.shape[1]
        el, _, fl = w1.shape
        cap = CF * k * tl // (el * nep)
        vm = pl.BlockSpec(memory_space=pltpu.VMEM)
        hbm = pl.BlockSpec(memory_space=pl.ANY)
        dma = pltpu.SemaphoreType.DMA
        nu = d // UN
        return pl.pallas_call(
            functools.partial(_moe_kernel, k, cap),
            out_shape=jax.ShapeDtypeStruct((tl, d), BF),
            in_specs=[hbm, vm, vm, hbm, hbm, hbm],
            out_specs=hbm,
            scratch_shapes=[
                pltpu.VMEM((nep, tl, d), BF),
                pltpu.VMEM((nep, 16, tl), F32),
                pltpu.VMEM((nep, el * cap, tl), BF),
                pltpu.VMEM((nep, 3, tl, el * cap), BF),
                pltpu.VMEM((el, nep * cap, CU), BF),
                pltpu.VMEM((el, 2 * fl, nep * cap), F32),
                pltpu.VMEM((el, nep * cap, fl), BF),
                pltpu.VMEM((SL, EB, 2 * fl, CU), BF),
                pltpu.VMEM((2, el, fl, NB), BF),
                pltpu.VMEM((8, nep, tl, NB), F32),
                pltpu.VMEM((2, 2, nep, tl, NB), F32),
                pltpu.VMEM((2, nep, tl, NB), F32),
                pltpu.VMEM((2, 5, tl, NB), F32),
                pltpu.VMEM((tl, NB), F32),
                pltpu.VMEM((tl, d), BF),
                dma((1,)),
                dma((2, 3)),
                dma((8, nu, 3)),
                dma((2, SL)),
                dma((2,)),
                dma((2, 2, 2, 4)),
                dma((2, 2, 4)),
                dma((2, 3)),
                dma((2, 5)),
                dma((2,)),
                dma((2, 2, 3)),
            ],
            compiler_params=pltpu.CompilerParams(
                collective_id=0, has_side_effects=True, vmem_limit_bytes=VMEM_LIMIT
            ),
        )(x, idx.T, g.T, w1.swapaxes(1, 2), w3.swapaxes(1, 2), w2)

    return jax.shard_map(
        body,
        mesh=mesh,
        in_specs=(tok, tok, tok, P("ep", None, "tp"), P("ep", None, "tp"), P("ep", "tp", None)),
        out_specs=tok,
        check_vma=False,
    )
```

```python
import functools

import jax
import jax.numpy as jnp
from jax import lax
from jax.experimental import pallas as pl
from jax.experimental.pallas import tpu as pltpu
from jax.sharding import PartitionSpec as P

MESH = pl.DeviceIdType.MESH
CF = 2
BF = jnp.bfloat16
F32 = jnp.float32
VMEM_LIMIT = 64 * 1000 * 1000


def _peers():
    z, t = lax.axis_index("ep"), lax.axis_index("tp")
    zs = (3 - z, lax.rem(z + 2, 4), z + 1 - 2 * lax.rem(z, 2))
    yq = lax.rem(t + 2, 4)
    cq = t + 1 - 2 * lax.rem(t, 2)
    return z, t, zs, yq, cq


def _entry_barrier(inner, zs, yq, cq):
    bar = pltpu.get_barrier_semaphore()

    @pl.when(inner)
    def _():
        pl.semaphore_signal(bar, inc=1, device_id={"ep": zs[0]}, device_id_type=MESH)

    for p in zs[1:]:
        pl.semaphore_signal(bar, inc=1, device_id={"ep": p}, device_id_type=MESH)
    for p in (yq, cq):
        pl.semaphore_signal(bar, inc=1, device_id={"tp": p}, device_id_type=MESH)
    z = lax.axis_index("ep")
    pl.semaphore_wait(bar, 4 + z * (3 - z) // 2)


def _rcopy(src, dst, ss, rs, dev):
    return pltpu.make_async_remote_copy(
        src_ref=src, dst_ref=dst, send_sem=ss, recv_sem=rs, device_id=dev, device_id_type=MESH
    )


def _members(rt, el, ebase, k):
    tl = rt.shape[1]
    eid = lax.broadcasted_iota(jnp.int32, (el, tl), 0) + ebase
    m = jnp.zeros((el, tl), F32)
    gm = jnp.zeros((el, tl), F32)
    for j in range(k):
        hit = rt[j : j + 1, :].astype(jnp.int32) == eid
        m = jnp.where(hit, 1.0, m)
        gm = jnp.where(hit, rt[8 + j : 9 + j, :], gm)
    a = lax.broadcasted_iota(jnp.int32, (tl, tl), 0)
    b = lax.broadcasted_iota(jnp.int32, (tl, tl), 1)
    u = jnp.where(a < b, 1.0, 0.0).astype(BF)
    slot = jnp.dot(m.astype(BF), u, preferred_element_type=F32)
    return jnp.where(m > 0, slot, -1.0), gm


NB = 256
UN = 256
CU = 512
FWD = {
    (0, 1): ((0, 4), (1, 1), (2, 3)),
    (0, 3): ((0, 5), (1, 2), (2, 4)),
    (1, 1): ((0, 6), (1, 3), (2, 5)),
    (1, 3): ((0, 7), (1, 4), (2, 6)),
    (2, 0): ((1, 5), (2, 7)),
    (2, 2): ((1, 6),),
    (3, 0): ((1, 7),),
}
UNITS = ((0, 1), (1, 2), (3, 2), (5, 2), (7, 1))
HR = 64
EB = 4
SL = 4
NT = (((1,), (1,)), ((), ()))


def _moe_kernel(
    k, cap, x_ref, id_ref, g_ref, w1_ref, w3_ref, w2_ref, y_ref,
    xb, rb, pm, gt, xe, hp, hb, wb, w2b, drecv, yrecv, zrecv, zfrecv, yb,
    lsem, rsem, xsem, xfsem, wsem, w2sem, dsem, ysem, zsem, zrsem, zfsem, fsem, hsem,
):
    z, t, zs, yq, cq = _peers()
    ns, tl, d = xb.shape
    el, fl = hb.shape[0], hb.shape[2]
    ebase = z * el
    nr = tl // 4
    nu = d // UN
    ng = el // EB
    side = z // 2
    inner = (z == 1) | (z == 2)

    def hacc(e):
        return hp.at[pl.ds(pl.multiple_of(e * 2 * fl, 2 * fl), 2 * fl), pl.ds(0, ns * cap)]

    def part(b, s):
        return hp.at[pl.ds(pl.multiple_of((b * ns + s) * tl, tl), tl), :]

    wsteps = [(j, g) for j in range(len(UNITS)) for g in range(ng)]

    def wcopies(step):
        j, g = wsteps[step]
        u0, n = UNITS[j]
        sl = step % SL
        cs, ws = pl.ds(u0 * UN, n * UN), pl.ds(0, n * UN)
        es = pl.ds(g * EB, EB)
        return (
            pltpu.make_async_copy(w1_ref.at[es, :, cs], wb.at[sl, :, pl.ds(0, fl), ws], wsem.at[0, sl]),
            pltpu.make_async_copy(w3_ref.at[es, :, cs], wb.at[sl, :, pl.ds(fl, fl), ws], wsem.at[1, sl]),
        )

    def wstart(step):
        for c in wcopies(step):
            c.start()

    own4 = (lax.rem(cq + 2, 4), yq, cq, t)
    cols = [own4[kd] * 512 + n * NB for n in range(2) for kd in range(4)]

    def w2copy(b):
        return pltpu.make_async_copy(
            w2_ref.at[:, :, pl.ds(pl.multiple_of(cols[b], NB), NB)], w2b.at[b % 2], w2sem.at[b % 2]
        )

    own = pltpu.make_async_copy(x_ref, xb.at[z], lsem.at[0])
    own.start()
    rb[z, 0:k] = id_ref[...].astype(F32)
    rb[z, 8 : 8 + k] = g_ref[...]
    for step in range(SL - 1):
        wstart(step)
    w2copy(0).start()
    w2copy(1).start()
    _entry_barrier(inner, zs, yq, cq)
    own.wait()

    def piece(c, s, q):
        return xb.at[s, pl.ds(pl.multiple_of(q * nr, nr), nr), pl.ds(pl.multiple_of(c * UN, UN), UN)]

    def xcopy(kind, c, i):
        p = zs[i]
        if kind == 0:
            r, dev = piece(c, z, t), {"ep": p}
        elif kind == 1:
            r, dev = piece(c, p, t), {"tp": yq}
        elif kind == 2:
            r, dev = piece(c, p, t), {"tp": cq}
        else:
            r, dev = piece(c, p, yq), {"tp": cq}
        return _rcopy(r, r, xsem.at[2 * kind, c, i], xsem.at[2 * kind + 1, c, i], dev)

    def rcopy(i):
        return _rcopy(rb.at[z], rb.at[z], rsem.at[0, i], rsem.at[1, i], {"ep": zs[i]})

    def xpass(c):
        r = piece(c, zs[1], t)
        return _rcopy(r, r, xfsem.at[c], xsem.at[1, c, 0], {"ep": zs[2]})

    def rpass():
        return _rcopy(rb.at[zs[1]], rb.at[zs[1]], rsem.at[0, 3], rsem.at[1, 0], {"ep": zs[2]})

    rcopy(1).start()
    xcopy(0, 0, 1).start()

    @pl.when(inner)
    def _():
        rcopy(0).start()
        xcopy(0, 0, 0).start()

    rcopy(2).start()
    xcopy(0, 0, 2).start()

    @pl.loop(1, nu)
    def _(c):
        xcopy(0, c, 1).start()

        @pl.when(inner)
        def _():
            xcopy(0, c, 0).start()

        xcopy(0, c, 2).start()

    def zhand(c, i):
        xcopy(0, c, i).wait_recv()
        if i == 1:

            @pl.when(inner)
            def _():
                xpass(c).start()

        xcopy(1, c, i).start()
        xcopy(2, c, i).start()

    def zfar(c):
        zhand(c, 1)

    def znear(c):
        zhand(c, 2)
        zhand(c, 0)

    def yforward(c):
        for i in (1, 2, 0):
            xcopy(1, c, i).wait_recv()
            xcopy(3, c, i).start()

    def xarrive(c):
        for i in range(3):
            xcopy(2, c, i).wait_recv()
            xcopy(3, c, i).wait_recv()

    ci = lax.broadcasted_iota(jnp.int32, (cap, tl), 0).astype(F32)

    def tables(s):
        slot, gm = _members(rb[s], el, ebase, k)
        gs = []
        for i in range(el):
            hit = slot[i : i + 1, :] == ci
            pm[s, i * cap : (i + 1) * cap, :] = jnp.where(hit, 1.0, 0.0).astype(BF)
            gs.append(jnp.where(hit, gm[i : i + 1, :], 0.0))
        g = jnp.concatenate(gs, axis=0).T
        hi = g.astype(BF)
        r = g - hi.astype(F32)
        mid = r.astype(BF)
        gt[s, 0] = hi
        gt[s, 1] = mid
        gt[s, 2] = (r - mid.astype(F32)).astype(BF)

    rcopy(1).wait_recv()

    @pl.when(inner)
    def _():
        rpass().start()

    zfar(0)
    rcopy(2).wait_recv()
    tables(z)
    zfar(1)
    znear(0)
    tables(zs[2])
    zfar(2)
    znear(1)
    rcopy(0).wait_recv()
    tables(zs[1])
    zfar(3)
    tables(zs[0])
    yforward(0)
    znear(2)

    for j, (u0, un) in enumerate(UNITS):
        for u in range(u0, u0 + un):
            xarrive(u)
        cs = pl.ds(u0 * UN, un * UN)
        for s in range(ns):
            v = jnp.dot(pm[s], xb[s, :, cs], preferred_element_type=F32).astype(BF)
            xe[:, s * cap : (s + 1) * cap, 0 : un * UN] = v.reshape(el, cap, un * UN)
        for g in range(ng):
            step = j * ng + g
            for f, u in FWD.get((j, g), ()):
                (zfar, yforward, znear)[f](u)
            for w in wcopies(step):
                w.wait()
            if step + SL - 1 < len(wsteps):
                wstart(step + SL - 1)
            for i in range(EB):
                e = g * EB + i
                v = lax.dot_general(
                    wb[step % SL, i, :, 0 : un * UN], xe[e, :, 0 : un * UN], NT, preferred_element_type=F32
                )
                if j > 0:
                    v += hacc(e)[...]
                if j < len(UNITS) - 1:
                    hacc(e)[...] = v
                else:
                    hb[e] = (jax.nn.silu(v[:fl]) * v[fl:]).T.astype(BF)

    def sof(i):
        far = (3 - i) * (1 - side) + i * side
        near = (i - 2) * z + (3 - i) * (1 - z + 4 * side)
        return far * (1 - i // 2) + near * (i // 2)

    def dcopy(n, j, i):
        s = sof(i)
        return _rcopy(
            part(n * 4 + 2 * j, s), drecv.at[n, j, s], dsem.at[0, n, j, i], dsem.at[1, n, j, i], {"tp": cq}
        )

    def ycopy(n, i):
        s = sof(i)
        return _rcopy(part(n * 4 + 1, s), yrecv.at[n, s], ysem.at[0, n, i], ysem.at[1, n, i], {"tp": yq})

    def zfirst():
        return _rcopy(part(1, sof(2)), zfrecv, zfsem.at[0], zfsem.at[1], {"ep": zs[2]})

    def compute(n, kd):
        b = n * 4 + kd
        w2copy(b).wait()
        sl = b % 2

        @pl.loop(0, el, step=8)
        def _(e0):
            for i in range(8):
                e = e0 + i
                v = jnp.dot(hb[e], w2b[sl, e], preferred_element_type=F32).astype(BF)
                pm[:, pl.ds(pl.multiple_of(e * cap, cap), cap), :] = v.reshape(ns, cap, NB)

        if b + 2 < 8:
            w2copy(b + 2).start()

        @pl.loop(0, ns)
        def _(i):
            s = sof(i)
            yp = pm[s]
            acc = jnp.dot(gt[s, 0], yp, preferred_element_type=F32)
            acc += jnp.dot(gt[s, 1], yp, preferred_element_type=F32)
            acc += jnp.dot(gt[s, 2], yp, preferred_element_type=F32)
            if kd % 2 == 0:
                part(b, s)[...] = acc
                dcopy(n, kd // 2, i).start()
            else:
                dcopy(n, kd // 2, i).wait_recv()
                part(b, s)[...] = acc + drecv[n, kd // 2, s]
                if kd == 1:

                    @pl.when(i < 2 + n)
                    def _():
                        ycopy(n, i).start()

                    if n == 0:

                        @pl.when(i == 2)
                        def _():
                            zfirst().start()

    def zdir(i):
        return side if i < 2 else lax.rem(z, 2)

    def zcopy(n, i):
        s, dr = sof(i), zdir(i)
        dn = z + 1 - 2 * dr
        slot = s - dn + 4 * dr
        return _rcopy(part(n * 4 + 3, s), zrecv.at[n, slot], zsem.at[n, i], zrsem.at[n, slot], {"ep": dn})

    def zarrive(n, s, slot):
        _rcopy(
            part(n * 4 + 3, s), zrecv.at[n, slot], zsem.at[n, 0], zrsem.at[n, slot], {"ep": zs[0]}
        ).wait_recv()
        part(n * 4 + 3, s)[...] += zrecv[n, slot]

    def hcopy(r):
        rs = pl.ds(r * HR, HR)
        return _rcopy(part(5, z).at[rs], yrecv.at[1, z, rs], hsem.at[0, r], hsem.at[1, r], {"tp": yq})

    def zacc(n, i):
        s = sof(i)
        if (n, i) != (0, 2):
            ycopy(n, i).wait_recv()
            part(n * 4 + 3, s)[...] += yrecv[n, s]
        if i < 3:

            @pl.when(~inner)
            def _():
                zcopy(n, i).start()

    def relay(n, i):
        @pl.when(inner)
        def _():
            s = sof(i)
            zarrive(n, s, s - z + 4 * zdir(i))
            zcopy(n, i).start()

    def fcopy(j, n, r=0):
        q, dev = ((t, yq), (t, cq), (yq, cq))[j]
        sl = pl.ds(pl.multiple_of(q * 512 + n * NB, NB), NB)
        rs = pl.ds(r * HR, HR) if n else pl.ds(0, tl)
        return _rcopy(yb.at[rs, sl], yb.at[rs, sl], fsem.at[0, n + r, j], fsem.at[1, n + r, j], {"tp": dev})

    pieces = ((0, 0),) + tuple((1, r) for r in range(tl // HR))

    def zfinish(n):
        @pl.when(z > 0)
        def _():
            zarrive(n, z, 0)

        @pl.when(z < 3)
        def _():
            zarrive(n, z, 4)

    def spread(n, r=0):
        rs = pl.ds(r * HR, HR) if n else pl.ds(0, tl)
        v = part(n * 4 + 3, z)[rs, :]
        if n:
            hcopy(r).wait_recv()
            v += yrecv[1, z, rs, :]
        yb[rs, pl.ds(pl.multiple_of(t * 512 + n * NB, NB), NB)] = v.astype(BF)
        fcopy(0, n, r).start()
        fcopy(1, n, r).start()

    compute(0, 0)
    compute(0, 1)
    compute(0, 2)
    compute(0, 3)
    zacc(0, 2)
    zacc(0, 0)
    compute(1, 0)
    compute(1, 1)
    zfirst().wait_recv()
    part(1, z)[...] += zfrecv[...]
    ycopy(0, 3).start()
    for r in range(tl // HR):
        hcopy(r).start()
    zacc(0, 1)
    relay(0, 0)
    compute(1, 2)
    compute(1, 3)
    relay(0, 1)
    zacc(1, 0)
    zacc(1, 1)
    relay(0, 2)
    relay(1, 0)
    zacc(1, 2)
    relay(1, 1)
    zacc(0, 3)
    relay(1, 2)
    zfinish(0)
    spread(0)
    zfinish(1)
    for n, r in pieces[1:]:
        spread(n, r)
    for n, r in pieces:
        fcopy(0, n, r).wait_recv()
        fcopy(2, n, r).start()

    @pl.loop(0, nu)
    def _(c):
        for kind in range(4):
            for i in range(3):
                if (kind, i) != (0, 0):
                    xcopy(kind, c, i).wait_send()

        @pl.when(inner)
        def _():
            xcopy(0, c, 0).wait_send()
            xpass(c).wait_send()

    rcopy(1).wait_send()
    rcopy(2).wait_send()

    @pl.when(inner)
    def _():
        rcopy(0).wait_send()
        rpass().wait_send()

    for n in range(2):
        for i in range(4):
            for j in range(2):
                dcopy(n, j, i).wait_send()
            if (n, i) not in ((0, 2), (1, 3)):
                ycopy(n, i).wait_send()
            if i < 3:
                zcopy(n, i).wait_send()
    zfirst().wait_send()
    for r in range(tl // HR):
        hcopy(r).wait_send()
    for n, r in pieces:
        fcopy(1, n, r).wait_recv()
        fcopy(2, n, r).wait_recv()
    for n, r in pieces:
        for j in range(3):
            fcopy(j, n, r).wait_send()
    out = pltpu.make_async_copy(yb, y_ref, lsem.at[0])
    out.start()
    out.wait()


def solution(mesh):
    tok = P(("dp", "ep"), None)
    nep = mesh.shape["ep"]

    def body(x, idx, g, w1, w3, w2):
        tl, d = x.shape
        k = idx.shape[1]
        el, _, fl = w1.shape
        cap = CF * k * tl // (el * nep)
        vm = pl.BlockSpec(memory_space=pltpu.VMEM)
        hbm = pl.BlockSpec(memory_space=pl.ANY)
        dma = pltpu.SemaphoreType.DMA
        nu = d // UN
        return pl.pallas_call(
            functools.partial(_moe_kernel, k, cap),
            out_shape=jax.ShapeDtypeStruct((tl, d), BF),
            in_specs=[hbm, vm, vm, hbm, hbm, hbm],
            out_specs=hbm,
            scratch_shapes=[
                pltpu.VMEM((nep, tl, d), BF),
                pltpu.VMEM((nep, 16, tl), F32),
                pltpu.VMEM((nep, el * cap, tl), BF),
                pltpu.VMEM((nep, 3, tl, el * cap), BF),
                pltpu.VMEM((el, nep * cap, CU), BF),
                pltpu.VMEM((el * 2 * fl, NB), F32),
                pltpu.VMEM((el, nep * cap, fl), BF),
                pltpu.VMEM((SL, EB, 2 * fl, CU), BF),
                pltpu.VMEM((2, el, fl, NB), BF),
                pltpu.VMEM((2, 2, nep, tl, NB), F32),
                pltpu.VMEM((2, nep, tl, NB), F32),
                pltpu.VMEM((2, 5, tl, NB), F32),
                pltpu.VMEM((tl, NB), F32),
                pltpu.VMEM((tl, d), BF),
                dma((1,)),
                dma((2, 4)),
                dma((8, nu, 3)),
                dma((nu,)),
                dma((2, SL)),
                dma((2,)),
                dma((2, 2, 2, 4)),
                dma((2, 2, 4)),
                dma((2, 3)),
                dma((2, 5)),
                dma((2,)),
                dma((2, 5, 3)),
                dma((2, tl // HR)),
            ],
            compiler_params=pltpu.CompilerParams(
                collective_id=0, has_side_effects=True, vmem_limit_bytes=VMEM_LIMIT
            ),
        )(x, idx.T, g.T, w1.swapaxes(1, 2), w3.swapaxes(1, 2), w2)

    return jax.shard_map(
        body,
        mesh=mesh,
        in_specs=(tok, tok, tok, P("ep", None, "tp"), P("ep", None, "tp"), P("ep", "tp", None)),
        out_specs=tok,
        check_vma=False,
    )
```

```python
import functools

import jax
import jax.numpy as jnp
from jax import lax
from jax.experimental import pallas as pl
from jax.experimental.pallas import tpu as pltpu
from jax.sharding import PartitionSpec as P

MESH = pl.DeviceIdType.MESH
CF = 2
BF = jnp.bfloat16
F32 = jnp.float32
VMEM_LIMIT = 64 * 1000 * 1000


def _peers():
    z, t = lax.axis_index("ep"), lax.axis_index("tp")
    zs = (3 - z, lax.rem(z + 2, 4), z + 1 - 2 * lax.rem(z, 2))
    yq = lax.rem(t + 2, 4)
    cq = t + 1 - 2 * lax.rem(t, 2)
    return z, t, zs, yq, cq


def _entry_barrier(inner, zs, yq, cq):
    bar = pltpu.get_barrier_semaphore()

    @pl.when(inner)
    def _():
        pl.semaphore_signal(bar, inc=1, device_id={"ep": zs[0]}, device_id_type=MESH)

    for p in zs[1:]:
        pl.semaphore_signal(bar, inc=1, device_id={"ep": p}, device_id_type=MESH)
    for p in (yq, cq):
        pl.semaphore_signal(bar, inc=1, device_id={"tp": p}, device_id_type=MESH)
    z = lax.axis_index("ep")
    pl.semaphore_wait(bar, 4 + z * (3 - z) // 2)


def _rcopy(src, dst, ss, rs, dev):
    return pltpu.make_async_remote_copy(
        src_ref=src, dst_ref=dst, send_sem=ss, recv_sem=rs, device_id=dev, device_id_type=MESH
    )


def _members(rt, el, ebase, k):
    tl = rt.shape[1]
    eid = lax.broadcasted_iota(jnp.int32, (el, tl), 0) + ebase
    m = jnp.zeros((el, tl), F32)
    gm = jnp.zeros((el, tl), F32)
    for j in range(k):
        hit = rt[j : j + 1, :].astype(jnp.int32) == eid
        m = jnp.where(hit, 1.0, m)
        gm = jnp.where(hit, rt[8 + j : 9 + j, :], gm)
    a = lax.broadcasted_iota(jnp.int32, (tl, tl), 0)
    b = lax.broadcasted_iota(jnp.int32, (tl, tl), 1)
    u = jnp.where(a < b, 1.0, 0.0).astype(BF)
    slot = jnp.dot(m.astype(BF), u, preferred_element_type=F32)
    return jnp.where(m > 0, slot, -1.0), gm


NB = 256
UN = 256
HR = 64
EB = 8
SL = 3
NT = (((1,), (1,)), ((), ()))


def _moe_kernel(
    k, cap, x_ref, id_ref, g_ref, w1_ref, w3_ref, w2_ref, y_ref,
    xb, rb, pm, gt, xe, hp, hb, wb, w2b, drecv, yrecv, zrecv, zfrecv, yb,
    lsem, rsem, xsem, xfsem, wsem, w2sem, dsem, ysem, zsem, zrsem, zfsem, fsem, hsem,
):
    z, t, zs, yq, cq = _peers()
    ns, tl, d = xb.shape
    el, fl = hb.shape[0], hb.shape[2]
    ebase = z * el
    nr = tl // 4
    nu = d // UN
    ng = el // EB
    side = z // 2
    inner = (z == 1) | (z == 2)

    def hacc(e):
        return hp.at[pl.ds(pl.multiple_of(e * 2 * fl, 2 * fl), 2 * fl), pl.ds(0, ns * cap)]

    def part(b, s):
        return hp.at[pl.ds(pl.multiple_of((b * ns + s) * tl, tl), tl), :]

    def wcopies(step):
        c, g = step // ng, lax.rem(step, ng)
        sl = lax.rem(step, SL)
        cs = pl.ds(pl.multiple_of(c * UN, UN), UN)
        es = pl.ds(g * EB, EB)
        return (
            pltpu.make_async_copy(w1_ref.at[es, :, cs], wb.at[sl, :, pl.ds(0, fl)], wsem.at[0, sl]),
            pltpu.make_async_copy(w3_ref.at[es, :, cs], wb.at[sl, :, pl.ds(fl, fl)], wsem.at[1, sl]),
        )

    def wstart(step):
        for c in wcopies(step):
            c.start()

    own4 = (lax.rem(cq + 2, 4), yq, cq, t)
    cols = [own4[kd] * 512 + n * NB for n in range(2) for kd in range(4)]

    def w2copy(b):
        return pltpu.make_async_copy(
            w2_ref.at[:, :, pl.ds(pl.multiple_of(cols[b], NB), NB)], w2b.at[b % 2], w2sem.at[b % 2]
        )

    own = pltpu.make_async_copy(x_ref, xb.at[z], lsem.at[0])
    own.start()
    rb[z, 0:k] = id_ref[...].astype(F32)
    rb[z, 8 : 8 + k] = g_ref[...]
    for step in range(SL - 1):
        wstart(step)
    w2copy(0).start()
    w2copy(1).start()
    _entry_barrier(inner, zs, yq, cq)
    own.wait()

    def piece(c, s, q):
        return xb.at[s, pl.ds(pl.multiple_of(q * nr, nr), nr), pl.ds(pl.multiple_of(c * UN, UN), UN)]

    def xcopy(kind, c, i):
        p = zs[i]
        if kind == 0:
            r, dev = piece(c, z, t), {"ep": p}
        elif kind == 1:
            r, dev = piece(c, p, t), {"tp": yq}
        elif kind == 2:
            r, dev = piece(c, p, t), {"tp": cq}
        else:
            r, dev = piece(c, p, yq), {"tp": cq}
        return _rcopy(r, r, xsem.at[2 * kind, c, i], xsem.at[2 * kind + 1, c, i], dev)

    def rcopy(i):
        return _rcopy(rb.at[z], rb.at[z], rsem.at[0, i], rsem.at[1, i], {"ep": zs[i]})

    def xpass(c):
        r = piece(c, zs[1], t)
        return _rcopy(r, r, xfsem.at[c], xsem.at[1, c, 0], {"ep": zs[2]})

    def rpass():
        return _rcopy(rb.at[zs[1]], rb.at[zs[1]], rsem.at[0, 3], rsem.at[1, 0], {"ep": zs[2]})

    rcopy(1).start()
    xcopy(0, 0, 1).start()

    @pl.when(inner)
    def _():
        rcopy(0).start()
        xcopy(0, 0, 0).start()

    rcopy(2).start()
    xcopy(0, 0, 2).start()

    @pl.loop(1, nu)
    def _(c):
        xcopy(0, c, 1).start()

        @pl.when(inner)
        def _():
            xcopy(0, c, 0).start()

        xcopy(0, c, 2).start()

    def zhand(c, i):
        xcopy(0, c, i).wait_recv()
        if i == 1:

            @pl.when(inner)
            def _():
                xpass(c).start()

        xcopy(1, c, i).start()
        xcopy(2, c, i).start()

    def zfar(c):
        zhand(c, 1)

    def znear(c):
        zhand(c, 2)
        zhand(c, 0)

    def yforward(c):
        for i in (1, 2, 0):
            xcopy(1, c, i).wait_recv()
            xcopy(3, c, i).start()

    def xarrive(c):
        for i in range(3):
            xcopy(2, c, i).wait_recv()
            xcopy(3, c, i).wait_recv()

    ci = lax.broadcasted_iota(jnp.int32, (cap, tl), 0).astype(F32)

    def tables(s):
        slot, gm = _members(rb[s], el, ebase, k)
        gs = []
        for i in range(el):
            hit = slot[i : i + 1, :] == ci
            pm[s, i * cap : (i + 1) * cap, :] = jnp.where(hit, 1.0, 0.0).astype(BF)
            gs.append(jnp.where(hit, gm[i : i + 1, :], 0.0))
        g = jnp.concatenate(gs, axis=0).T
        hi = g.astype(BF)
        r = g - hi.astype(F32)
        mid = r.astype(BF)
        gt[s, 0] = hi
        gt[s, 1] = mid
        gt[s, 2] = (r - mid.astype(F32)).astype(BF)

    rcopy(1).wait_recv()

    @pl.when(inner)
    def _():
        rpass().start()

    zfar(0)
    rcopy(2).wait_recv()
    tables(z)
    zfar(1)
    znear(0)
    tables(zs[2])
    zfar(2)
    znear(1)
    rcopy(0).wait_recv()
    tables(zs[1])
    zfar(3)
    tables(zs[0])
    yforward(0)
    znear(2)

    def when(cond, f):
        if isinstance(cond, bool):
            if cond:
                f()
        else:
            pl.when(cond)(f)

    def multiply(u, first, last):
        xarrive(u)
        cs = pl.ds(pl.multiple_of(u * UN, UN), UN)
        for s in range(ns):
            v = jnp.dot(pm[s], xb[s, :, cs], preferred_element_type=F32).astype(BF)
            xe[:, s * cap : (s + 1) * cap, :] = v.reshape(el, cap, UN)
        for g in range(ng):
            step = u * ng + g
            if g == ng - 1 and not last:
                when(u + 4 < nu, lambda: zfar(u + 4))
                yforward(u + 1)
                when(u + 3 < nu, lambda: znear(u + 3))
            for w in wcopies(step):
                w.wait()
            when(step + SL - 1 < nu * ng, lambda: wstart(step + SL - 1))
            sl = lax.rem(step, SL)
            for i in range(EB):
                e = g * EB + i
                v = lax.dot_general(wb[sl, i], xe[e], NT, preferred_element_type=F32)
                if not first:
                    v += hacc(e)[...]
                if not last:
                    hacc(e)[...] = v
                else:
                    hb[e] = (jax.nn.silu(v[:fl]) * v[fl:]).T.astype(BF)

    multiply(0, True, False)

    @pl.loop(1, nu - 1)
    def _(u):
        multiply(u, False, False)

    multiply(nu - 1, False, True)

    def sof(i):
        far = (3 - i) * (1 - side) + i * side
        near = (i - 2) * z + (3 - i) * (1 - z + 4 * side)
        return far * (1 - i // 2) + near * (i // 2)

    def dcopy(n, j, i):
        s = sof(i)
        return _rcopy(
            part(n * 4 + 2 * j, s), drecv.at[n, j, s], dsem.at[0, n, j, i], dsem.at[1, n, j, i], {"tp": cq}
        )

    def ycopy(n, i):
        s = sof(i)
        return _rcopy(part(n * 4 + 1, s), yrecv.at[n, s], ysem.at[0, n, i], ysem.at[1, n, i], {"tp": yq})

    def zfirst():
        return _rcopy(part(1, sof(2)), zfrecv, zfsem.at[0], zfsem.at[1], {"ep": zs[2]})

    def compute(n, kd):
        b = n * 4 + kd
        w2copy(b).wait()
        sl = b % 2

        @pl.loop(0, el, step=8)
        def _(e0):
            for i in range(8):
                e = e0 + i
                v = jnp.dot(hb[e], w2b[sl, e], preferred_element_type=F32).astype(BF)
                pm[:, pl.ds(pl.multiple_of(e * cap, cap), cap), :] = v.reshape(ns, cap, NB)

        if b + 2 < 8:
            w2copy(b + 2).start()

        @pl.loop(0, ns)
        def _(i):
            s = sof(i)
            yp = pm[s]
            acc = jnp.dot(gt[s, 0], yp, preferred_element_type=F32)
            acc += jnp.dot(gt[s, 1], yp, preferred_element_type=F32)
            acc += jnp.dot(gt[s, 2], yp, preferred_element_type=F32)
            if kd % 2 == 0:
                part(b, s)[...] = acc
                dcopy(n, kd // 2, i).start()
            else:
                dcopy(n, kd // 2, i).wait_recv()
                part(b, s)[...] = acc + drecv[n, kd // 2, s]
                if kd == 1:

                    @pl.when(i < 2 + n)
                    def _():
                        ycopy(n, i).start()

                    if n == 0:

                        @pl.when(i == 2)
                        def _():
                            zfirst().start()

    def zdir(i):
        return side if i < 2 else lax.rem(z, 2)

    def zcopy(n, i):
        s, dr = sof(i), zdir(i)
        dn = z + 1 - 2 * dr
        slot = s - dn + 4 * dr
        return _rcopy(part(n * 4 + 3, s), zrecv.at[n, slot], zsem.at[n, i], zrsem.at[n, slot], {"ep": dn})

    def zarrive(n, s, slot):
        _rcopy(
            part(n * 4 + 3, s), zrecv.at[n, slot], zsem.at[n, 0], zrsem.at[n, slot], {"ep": zs[0]}
        ).wait_recv()
        part(n * 4 + 3, s)[...] += zrecv[n, slot]

    def hcopy(r):
        rs = pl.ds(r * HR, HR)
        return _rcopy(part(5, z).at[rs], yrecv.at[1, z, rs], hsem.at[0, r], hsem.at[1, r], {"tp": yq})

    def zacc(n, i):
        s = sof(i)
        if (n, i) != (0, 2):
            ycopy(n, i).wait_recv()
            part(n * 4 + 3, s)[...] += yrecv[n, s]
        if i < 3:

            @pl.when(~inner)
            def _():
                zcopy(n, i).start()

    def relay(n, i):
        @pl.when(inner)
        def _():
            s = sof(i)
            zarrive(n, s, s - z + 4 * zdir(i))
            zcopy(n, i).start()

    def fcopy(j, n, r=0):
        q, dev = ((t, yq), (t, cq), (yq, cq))[j]
        sl = pl.ds(pl.multiple_of(q * 512 + n * NB, NB), NB)
        rs = pl.ds(r * HR, HR) if n else pl.ds(0, tl)
        return _rcopy(yb.at[rs, sl], yb.at[rs, sl], fsem.at[0, n + r, j], fsem.at[1, n + r, j], {"tp": dev})

    pieces = ((0, 0),) + tuple((1, r) for r in range(tl // HR))

    def zfinish(n):
        @pl.when(z > 0)
        def _():
            zarrive(n, z, 0)

        @pl.when(z < 3)
        def _():
            zarrive(n, z, 4)

    def spread(n, r=0):
        rs = pl.ds(r * HR, HR) if n else pl.ds(0, tl)
        v = part(n * 4 + 3, z)[rs, :]
        if n:
            hcopy(r).wait_recv()
            v += yrecv[1, z, rs, :]
        yb[rs, pl.ds(pl.multiple_of(t * 512 + n * NB, NB), NB)] = v.astype(BF)
        fcopy(0, n, r).start()
        fcopy(1, n, r).start()

    compute(0, 0)
    compute(0, 1)
    compute(0, 2)
    compute(0, 3)
    zacc(0, 0)
    compute(1, 0)
    compute(1, 1)
    zfirst().wait_recv()
    part(1, z)[...] += zfrecv[...]
    ycopy(0, 3).start()
    for r in range(tl // HR):
        hcopy(r).start()
    zacc(0, 1)
    relay(0, 0)
    compute(1, 2)
    compute(1, 3)
    zacc(1, 0)
    relay(0, 1)
    zacc(1, 1)
    relay(1, 0)
    zacc(0, 2)
    relay(0, 2)
    zacc(1, 2)
    relay(1, 1)
    zacc(0, 3)
    relay(1, 2)
    zfinish(0)
    spread(0)
    zfinish(1)
    for n, r in pieces[1:]:
        spread(n, r)
    for n, r in pieces:
        fcopy(0, n, r).wait_recv()
        fcopy(2, n, r).start()

    @pl.loop(0, nu)
    def _(c):
        for kind in range(4):
            for i in range(3):
                if (kind, i) != (0, 0):
                    xcopy(kind, c, i).wait_send()

        @pl.when(inner)
        def _():
            xcopy(0, c, 0).wait_send()
            xpass(c).wait_send()

    rcopy(1).wait_send()
    rcopy(2).wait_send()

    @pl.when(inner)
    def _():
        rcopy(0).wait_send()
        rpass().wait_send()

    for n in range(2):
        for i in range(4):
            for j in range(2):
                dcopy(n, j, i).wait_send()
            if (n, i) not in ((0, 2), (1, 3)):
                ycopy(n, i).wait_send()
            if i < 3:
                zcopy(n, i).wait_send()
    zfirst().wait_send()
    for r in range(tl // HR):
        hcopy(r).wait_send()
    for n, r in pieces:
        fcopy(1, n, r).wait_recv()
        fcopy(2, n, r).wait_recv()
    for n, r in pieces:
        for j in range(3):
            fcopy(j, n, r).wait_send()
    out = pltpu.make_async_copy(yb, y_ref, lsem.at[0])
    out.start()
    out.wait()


def solution(mesh):
    tok = P(("dp", "ep"), None)
    nep = mesh.shape["ep"]

    def body(x, idx, g, w1, w3, w2):
        tl, d = x.shape
        k = idx.shape[1]
        el, _, fl = w1.shape
        cap = CF * k * tl // (el * nep)
        vm = pl.BlockSpec(memory_space=pltpu.VMEM)
        hbm = pl.BlockSpec(memory_space=pl.ANY)
        dma = pltpu.SemaphoreType.DMA
        nu = d // UN
        return pl.pallas_call(
            functools.partial(_moe_kernel, k, cap),
            out_shape=jax.ShapeDtypeStruct((tl, d), BF),
            in_specs=[hbm, vm, vm, hbm, hbm, hbm],
            out_specs=hbm,
            scratch_shapes=[
                pltpu.VMEM((nep, tl, d), BF),
                pltpu.VMEM((nep, 16, tl), F32),
                pltpu.VMEM((nep, el * cap, tl), BF),
                pltpu.VMEM((nep, 3, tl, el * cap), BF),
                pltpu.VMEM((el, nep * cap, UN), BF),
                pltpu.VMEM((el * 2 * fl, NB), F32),
                pltpu.VMEM((el, nep * cap, fl), BF),
                pltpu.VMEM((SL, EB, 2 * fl, UN), BF),
                pltpu.VMEM((2, el, fl, NB), BF),
                pltpu.VMEM((2, 2, nep, tl, NB), F32),
                pltpu.VMEM((2, nep, tl, NB), F32),
                pltpu.VMEM((2, 5, tl, NB), F32),
                pltpu.VMEM((tl, NB), F32),
                pltpu.VMEM((tl, d), BF),
                dma((1,)),
                dma((2, 4)),
                dma((8, nu, 3)),
                dma((nu,)),
                dma((2, SL)),
                dma((2,)),
                dma((2, 2, 2, 4)),
                dma((2, 2, 4)),
                dma((2, 3)),
                dma((2, 5)),
                dma((2,)),
                dma((2, 5, 3)),
                dma((2, tl // HR)),
            ],
            compiler_params=pltpu.CompilerParams(
                collective_id=0, has_side_effects=True, vmem_limit_bytes=VMEM_LIMIT
            ),
        )(x, idx.T, g.T, w1.swapaxes(1, 2), w3.swapaxes(1, 2), w2)

    return jax.shard_map(
        body,
        mesh=mesh,
        in_specs=(tok, tok, tok, P("ep", None, "tp"), P("ep", None, "tp"), P("ep", "tp", None)),
        out_specs=tok,
        check_vma=False,
    )
```

```python
import functools

import jax
import jax.numpy as jnp
from jax import lax
from jax.experimental import pallas as pl
from jax.experimental.pallas import tpu as pltpu
from jax.sharding import PartitionSpec as P

MESH = pl.DeviceIdType.MESH
CF = 2
BF = jnp.bfloat16
F32 = jnp.float32
VMEM_LIMIT = 64 * 1000 * 1000


def _peers():
    z, t = lax.axis_index("ep"), lax.axis_index("tp")
    zs = (3 - z, lax.rem(z + 2, 4), z + 1 - 2 * lax.rem(z, 2))
    yq = lax.rem(t + 2, 4)
    cq = t + 1 - 2 * lax.rem(t, 2)
    return z, t, zs, yq, cq


def _entry_barrier(inner, zs, yq, cq):
    bar = pltpu.get_barrier_semaphore()

    @pl.when(inner)
    def _():
        pl.semaphore_signal(bar, inc=1, device_id={"ep": zs[0]}, device_id_type=MESH)

    for p in zs[1:]:
        pl.semaphore_signal(bar, inc=1, device_id={"ep": p}, device_id_type=MESH)
    for p in (yq, cq):
        pl.semaphore_signal(bar, inc=1, device_id={"tp": p}, device_id_type=MESH)
    z = lax.axis_index("ep")
    pl.semaphore_wait(bar, 4 + z * (3 - z) // 2)


def _rcopy(src, dst, ss, rs, dev):
    return pltpu.make_async_remote_copy(
        src_ref=src, dst_ref=dst, send_sem=ss, recv_sem=rs, device_id=dev, device_id_type=MESH
    )


def _members(rt, el, ebase, k):
    tl = rt.shape[1]
    eid = lax.broadcasted_iota(jnp.int32, (el, tl), 0) + ebase
    m = jnp.zeros((el, tl), F32)
    gm = jnp.zeros((el, tl), F32)
    for j in range(k):
        hit = rt[j : j + 1, :].astype(jnp.int32) == eid
        m = jnp.where(hit, 1.0, m)
        gm = jnp.where(hit, rt[8 + j : 9 + j, :], gm)
    a = lax.broadcasted_iota(jnp.int32, (tl, tl), 0)
    b = lax.broadcasted_iota(jnp.int32, (tl, tl), 1)
    u = jnp.where(a < b, 1.0, 0.0).astype(BF)
    slot = jnp.dot(m.astype(BF), u, preferred_element_type=F32)
    return jnp.where(m > 0, slot, -1.0), gm


NB = 256
UN = 256
HR = 64
EB = 8
SL = 3
NT = (((1,), (1,)), ((), ()))


def _moe_kernel(
    k, cap, x_ref, id_ref, g_ref, w1_ref, w3_ref, w2_ref, y_ref,
    xb, rb, pm, gt, xe, hp, hb, wb, w2b, drecv, yrecv, zrecv, zfrecv, yb,
    lsem, rsem, xsem, xfsem, wsem, w2sem, dsem, ysem, zsem, zrsem, zfsem, fsem, hsem,
):
    z, t, zs, yq, cq = _peers()
    ns, tl, d = xb.shape
    el, fl = hb.shape[0], hb.shape[2]
    ebase = z * el
    nr = tl // 4
    nu = d // UN
    ng = el // EB
    side = z // 2
    inner = (z == 1) | (z == 2)

    def hacc(e):
        return hp.at[pl.ds(pl.multiple_of(e * 2 * fl, 2 * fl), 2 * fl), pl.ds(0, ns * cap)]

    def part(b, s):
        return hp.at[pl.ds(pl.multiple_of((b * ns + s) * tl, tl), tl), :]

    def wcopies(step):
        c, g = step // ng, lax.rem(step, ng)
        sl = lax.rem(step, SL)
        cs = pl.ds(pl.multiple_of(c * UN, UN), UN)
        es = pl.ds(g * EB, EB)
        return (
            pltpu.make_async_copy(w1_ref.at[es, :, cs], wb.at[sl, :, pl.ds(0, fl)], wsem.at[0, sl]),
            pltpu.make_async_copy(w3_ref.at[es, :, cs], wb.at[sl, :, pl.ds(fl, fl)], wsem.at[1, sl]),
        )

    def wstart(step):
        for c in wcopies(step):
            c.start()

    own4 = (lax.rem(cq + 2, 4), yq, cq, t)
    cols = [own4[kd] * 512 + n * NB for n in range(2) for kd in range(4)]

    def w2copy(b):
        return pltpu.make_async_copy(
            w2_ref.at[:, :, pl.ds(pl.multiple_of(cols[b], NB), NB)], w2b.at[b % 2], w2sem.at[b % 2]
        )

    own = pltpu.make_async_copy(x_ref, xb.at[z], lsem.at[0])
    own.start()
    rb[z, 0:k] = id_ref[...].astype(F32)
    rb[z, 8 : 8 + k] = g_ref[...]
    for step in range(SL - 1):
        wstart(step)
    w2copy(0).start()
    w2copy(1).start()
    _entry_barrier(inner, zs, yq, cq)
    own.wait()

    def piece(c, s, q):
        return xb.at[s, pl.ds(pl.multiple_of(q * nr, nr), nr), pl.ds(pl.multiple_of(c * UN, UN), UN)]

    def xcopy(kind, c, i):
        p = zs[i]
        if kind == 0:
            r, dev = piece(c, z, t), {"ep": p}
        elif kind == 1:
            r, dev = piece(c, p, t), {"tp": yq}
        elif kind == 2:
            r, dev = piece(c, p, t), {"tp": cq}
        else:
            r, dev = piece(c, p, yq), {"tp": cq}
        return _rcopy(r, r, xsem.at[2 * kind, c, i], xsem.at[2 * kind + 1, c, i], dev)

    def rcopy(i):
        return _rcopy(rb.at[z], rb.at[z], rsem.at[0, i], rsem.at[1, i], {"ep": zs[i]})

    def xpass(c):
        r = piece(c, zs[1], t)
        return _rcopy(r, r, xfsem.at[c], xsem.at[1, c, 0], {"ep": zs[2]})

    def rpass():
        return _rcopy(rb.at[zs[1]], rb.at[zs[1]], rsem.at[0, 3], rsem.at[1, 0], {"ep": zs[2]})

    rcopy(1).start()
    xcopy(0, 0, 1).start()

    @pl.when(inner)
    def _():
        rcopy(0).start()
        xcopy(0, 0, 0).start()

    rcopy(2).start()
    xcopy(0, 0, 2).start()

    @pl.loop(1, nu)
    def _(c):
        xcopy(0, c, 1).start()

        @pl.when(inner)
        def _():
            xcopy(0, c, 0).start()

        xcopy(0, c, 2).start()

    def zhand(c, i):
        xcopy(0, c, i).wait_recv()
        if i == 1:

            @pl.when(inner)
            def _():
                xpass(c).start()

        xcopy(1, c, i).start()
        xcopy(2, c, i).start()

    def zfar(c):
        zhand(c, 1)

    def znear(c):
        zhand(c, 2)
        zhand(c, 0)

    def yforward(c):
        for i in (1, 2, 0):
            xcopy(1, c, i).wait_recv()
            xcopy(3, c, i).start()

    def xarrive(c):
        for i in range(3):
            xcopy(2, c, i).wait_recv()
            xcopy(3, c, i).wait_recv()

    ci = lax.broadcasted_iota(jnp.int32, (cap, tl), 0).astype(F32)

    def tables(s):
        slot, gm = _members(rb[s], el, ebase, k)
        gs = []
        for i in range(el):
            hit = slot[i : i + 1, :] == ci
            pm[s, i * cap : (i + 1) * cap, :] = jnp.where(hit, 1.0, 0.0).astype(BF)
            gs.append(jnp.where(hit, gm[i : i + 1, :], 0.0))
        g = jnp.concatenate(gs, axis=0).T
        hi = g.astype(BF)
        r = g - hi.astype(F32)
        mid = r.astype(BF)
        gt[s, 0] = hi
        gt[s, 1] = mid
        gt[s, 2] = (r - mid.astype(F32)).astype(BF)

    rcopy(1).wait_recv()

    @pl.when(inner)
    def _():
        rpass().start()

    zfar(0)
    rcopy(2).wait_recv()
    tables(z)
    zfar(1)
    znear(0)
    tables(zs[2])
    zfar(2)
    znear(1)
    rcopy(0).wait_recv()
    tables(zs[1])
    zfar(3)
    tables(zs[0])
    yforward(0)
    znear(2)

    def when(cond, f):
        if isinstance(cond, bool):
            if cond:
                f()
        else:
            pl.when(cond)(f)

    def multiply(u, first, last):
        xarrive(u)
        cs = pl.ds(pl.multiple_of(u * UN, UN), UN)
        for s in range(ns):
            v = jnp.dot(pm[s], xb[s, :, cs], preferred_element_type=F32).astype(BF)
            xe[:, s * cap : (s + 1) * cap, :] = v.reshape(el, cap, UN)
        for g in range(ng):
            step = u * ng + g
            if g == ng - 1 and not last:
                yforward(u + 1)
                when(u + 4 < nu, lambda: zfar(u + 4))
                when(u + 3 < nu, lambda: znear(u + 3))
            for w in wcopies(step):
                w.wait()
            when(step + SL - 1 < nu * ng, lambda: wstart(step + SL - 1))
            sl = lax.rem(step, SL)
            for i in range(EB):
                e = g * EB + i
                v = lax.dot_general(wb[sl, i], xe[e], NT, preferred_element_type=F32)
                if not first:
                    v += hacc(e)[...]
                if not last:
                    hacc(e)[...] = v
                else:
                    hb[e] = (jax.nn.silu(v[:fl]) * v[fl:]).T.astype(BF)

    multiply(0, True, False)

    @pl.loop(1, nu - 1)
    def _(u):
        multiply(u, False, False)

    multiply(nu - 1, False, True)

    def sof(i):
        far = (3 - i) * (1 - side) + i * side
        near = (i - 2) * z + (3 - i) * (1 - z + 4 * side)
        return far * (1 - i // 2) + near * (i // 2)

    def dcopy(n, j, i):
        s = sof(i)
        return _rcopy(
            part(n * 4 + 2 * j, s), drecv.at[n, j, s], dsem.at[0, n, j, i], dsem.at[1, n, j, i], {"tp": cq}
        )

    def ycopy(n, i):
        s = sof(i)
        return _rcopy(part(n * 4 + 1, s), yrecv.at[n, s], ysem.at[0, n, i], ysem.at[1, n, i], {"tp": yq})

    def zfirst():
        return _rcopy(part(1, sof(2)), zfrecv, zfsem.at[0], zfsem.at[1], {"ep": zs[2]})

    def compute(n, kd):
        b = n * 4 + kd
        w2copy(b).wait()
        sl = b % 2

        @pl.loop(0, el, step=16)
        def _(e0):
            for i in range(16):
                e = e0 + i
                v = jnp.dot(hb[e], w2b[sl, e], preferred_element_type=F32).astype(BF)
                pm[:, pl.ds(pl.multiple_of(e * cap, cap), cap), :] = v.reshape(ns, cap, NB)

        if b + 2 < 8:
            w2copy(b + 2).start()

        @pl.loop(0, ns)
        def _(i):
            s = sof(i)
            yp = pm[s]
            acc = jnp.dot(gt[s, 0], yp, preferred_element_type=F32)
            acc += jnp.dot(gt[s, 1], yp, preferred_element_type=F32)
            acc += jnp.dot(gt[s, 2], yp, preferred_element_type=F32)
            if kd % 2 == 0:
                part(b, s)[...] = acc
                dcopy(n, kd // 2, i).start()
            else:
                dcopy(n, kd // 2, i).wait_recv()
                part(b, s)[...] = acc + drecv[n, kd // 2, s]
                if kd == 1:

                    @pl.when(i < 2 + n)
                    def _():
                        ycopy(n, i).start()

                    if n == 0:

                        @pl.when(i == 2)
                        def _():
                            zfirst().start()

    def zdir(i):
        return side if i < 2 else lax.rem(z, 2)

    def zcopy(n, i):
        s, dr = sof(i), zdir(i)
        dn = z + 1 - 2 * dr
        slot = s - dn + 4 * dr
        return _rcopy(part(n * 4 + 3, s), zrecv.at[n, slot], zsem.at[n, i], zrsem.at[n, slot], {"ep": dn})

    def zarrive(n, s, slot):
        _rcopy(
            part(n * 4 + 3, s), zrecv.at[n, slot], zsem.at[n, 0], zrsem.at[n, slot], {"ep": zs[0]}
        ).wait_recv()
        part(n * 4 + 3, s)[...] += zrecv[n, slot]

    def hcopy(r):
        rs = pl.ds(r * HR, HR)
        return _rcopy(part(5, z).at[rs], yrecv.at[1, z, rs], hsem.at[0, r], hsem.at[1, r], {"tp": yq})

    def zacc(n, i):
        s = sof(i)
        if (n, i) != (0, 2):
            ycopy(n, i).wait_recv()
            part(n * 4 + 3, s)[...] += yrecv[n, s]
        if i < 3:

            @pl.when(~inner)
            def _():
                zcopy(n, i).start()

    def relay(n, i):
        @pl.when(inner)
        def _():
            s = sof(i)
            zarrive(n, s, s - z + 4 * zdir(i))
            zcopy(n, i).start()

    def fcopy(j, n, r=0):
        q, dev = ((t, yq), (t, cq), (yq, cq))[j]
        sl = pl.ds(pl.multiple_of(q * 512 + n * NB, NB), NB)
        rs = pl.ds(r * HR, HR) if n else pl.ds(0, tl)
        return _rcopy(yb.at[rs, sl], yb.at[rs, sl], fsem.at[0, n + r, j], fsem.at[1, n + r, j], {"tp": dev})

    pieces = ((0, 0),) + tuple((1, r) for r in range(tl // HR))

    def zfinish(n):
        @pl.when(z > 0)
        def _():
            zarrive(n, z, 0)

        @pl.when(z < 3)
        def _():
            zarrive(n, z, 4)

    def spread(n, r=0):
        rs = pl.ds(r * HR, HR) if n else pl.ds(0, tl)
        v = part(n * 4 + 3, z)[rs, :]
        if n:
            hcopy(r).wait_recv()
            v += yrecv[1, z, rs, :]
        yb[rs, pl.ds(pl.multiple_of(t * 512 + n * NB, NB), NB)] = v.astype(BF)
        fcopy(0, n, r).start()
        fcopy(1, n, r).start()

    compute(0, 0)
    compute(0, 1)
    compute(0, 2)
    compute(0, 3)
    zacc(0, 0)
    compute(1, 0)
    compute(1, 1)
    zfirst().wait_recv()
    part(1, z)[...] += zfrecv[...]
    ycopy(0, 3).start()
    for r in range(tl // HR):
        hcopy(r).start()
    zacc(0, 1)
    relay(0, 0)
    compute(1, 2)
    compute(1, 3)
    zacc(1, 0)
    relay(0, 1)
    zacc(1, 1)
    relay(1, 0)
    zacc(0, 2)
    relay(0, 2)
    zacc(1, 2)
    relay(1, 1)
    zacc(0, 3)
    relay(1, 2)
    zfinish(0)
    spread(0)
    zfinish(1)
    for n, r in pieces[1:]:
        spread(n, r)
    for n, r in pieces:
        fcopy(0, n, r).wait_recv()
        fcopy(2, n, r).start()

    @pl.loop(0, nu)
    def _(c):
        for kind in range(4):
            for i in range(3):
                if (kind, i) != (0, 0):
                    xcopy(kind, c, i).wait_send()

        @pl.when(inner)
        def _():
            xcopy(0, c, 0).wait_send()
            xpass(c).wait_send()

    rcopy(1).wait_send()
    rcopy(2).wait_send()

    @pl.when(inner)
    def _():
        rcopy(0).wait_send()
        rpass().wait_send()

    for n in range(2):
        for i in range(4):
            for j in range(2):
                dcopy(n, j, i).wait_send()
            if (n, i) not in ((0, 2), (1, 3)):
                ycopy(n, i).wait_send()
            if i < 3:
                zcopy(n, i).wait_send()
    zfirst().wait_send()
    for r in range(tl // HR):
        hcopy(r).wait_send()
    for n, r in pieces:
        fcopy(1, n, r).wait_recv()
        fcopy(2, n, r).wait_recv()
    for n, r in pieces:
        for j in range(3):
            fcopy(j, n, r).wait_send()
    out = pltpu.make_async_copy(yb, y_ref, lsem.at[0])
    out.start()
    out.wait()


def solution(mesh):
    tok = P(("dp", "ep"), None)
    nep = mesh.shape["ep"]

    def body(x, idx, g, w1, w3, w2):
        tl, d = x.shape
        k = idx.shape[1]
        el, _, fl = w1.shape
        cap = CF * k * tl // (el * nep)
        vm = pl.BlockSpec(memory_space=pltpu.VMEM)
        hbm = pl.BlockSpec(memory_space=pl.ANY)
        dma = pltpu.SemaphoreType.DMA
        nu = d // UN
        return pl.pallas_call(
            functools.partial(_moe_kernel, k, cap),
            out_shape=jax.ShapeDtypeStruct((tl, d), BF),
            in_specs=[hbm, vm, vm, hbm, hbm, hbm],
            out_specs=hbm,
            scratch_shapes=[
                pltpu.VMEM((nep, tl, d), BF),
                pltpu.VMEM((nep, 16, tl), F32),
                pltpu.VMEM((nep, el * cap, tl), BF),
                pltpu.VMEM((nep, 3, tl, el * cap), BF),
                pltpu.VMEM((el, nep * cap, UN), BF),
                pltpu.VMEM((el * 2 * fl, NB), F32),
                pltpu.VMEM((el, nep * cap, fl), BF),
                pltpu.VMEM((SL, EB, 2 * fl, UN), BF),
                pltpu.VMEM((2, el, fl, NB), BF),
                pltpu.VMEM((2, 2, nep, tl, NB), F32),
                pltpu.VMEM((2, nep, tl, NB), F32),
                pltpu.VMEM((2, 5, tl, NB), F32),
                pltpu.VMEM((tl, NB), F32),
                pltpu.VMEM((tl, d), BF),
                dma((1,)),
                dma((2, 4)),
                dma((8, nu, 3)),
                dma((nu,)),
                dma((2, SL)),
                dma((2,)),
                dma((2, 2, 2, 4)),
                dma((2, 2, 4)),
                dma((2, 3)),
                dma((2, 5)),
                dma((2,)),
                dma((2, 5, 3)),
                dma((2, tl // HR)),
            ],
            compiler_params=pltpu.CompilerParams(
                collective_id=0, has_side_effects=True, vmem_limit_bytes=VMEM_LIMIT
            ),
        )(x, idx.T, g.T, w1.swapaxes(1, 2), w3.swapaxes(1, 2), w2)

    return jax.shard_map(
        body,
        mesh=mesh,
        in_specs=(tok, tok, tok, P("ep", None, "tp"), P("ep", None, "tp"), P("ep", "tp", None)),
        out_specs=tok,
        check_vma=False,
    )
```
